256 devices in a mesh: image: 16 (over z, x_lo), space: 16 (over x_hi, y, core).
Axes of the slice: x: 4 (x_hi: 2, x_lo: 2; x = x_hi * 2 + x_lo), y: 4, z: 8, core: 2. Of those that a mesh axis runs over, the one named last changes fastest.
Arguments:
- magnet: float32 [32, 3, 8, 256, 256], P('image', None, None, 'space'), may hold values from -1 to 1, as said below
- anisotropy: float32 [256], P('space'), may hold values from 0.25 to 10
- kernel: float32 [6, 16, 512, 512], P(None, 'space'), as said below
Outputs:
- updated_magnet: float32 [32, 3, 8, 256, 256], P('image', None, None, 'space')
- band_force: float32 [32, 3, 8, 256, 256], P('image', None, None, 'space')
- energy: float32 [32], P('image')
The draws below stay inside these ranges and needn't reach their ends.
Inputs may be any that keep to these rules, and one draw needn't show every extreme that they name: `magnet`: each cell's three components form a unit vector. `kernel`: each component is even under k -> -k modulo the padded length along every frequency index, except that xy is odd along x and y, xz odd along x and z, and yz odd along y and z.
All inputs are finite; a program needn't handle non-finite values.
Results may differ from the reference program's by a relative error of at most 0.0003.
Values sent between devices are 32-bit elements; how exact they have to be, the bound alone decides.
A program may use at most 128 MiB of HBM per device.

```python
import math
import jax
import jax.numpy as jnp
from jax import lax

NX = 256
NY = 256
NZ = 8
IMAGES = 32


def mirror_part(values, dimension, parity):
    mirrored = jnp.roll(jnp.flip(values, dimension), 1, dimension)
    return 0.5 * (values + parity * mirrored)


def draw_kernel(key, part):
    array_dims = (6, 2 * NZ, 2 * NX, 2 * NY)
    samples = jax.random.normal(key, array_dims, jnp.float32)
    parities = ((1.0, 1.0, 1.0), (1.0, 1.0, 1.0), (1.0, 1.0, 1.0), (-1.0, -1.0, 1.0), (-1.0, 1.0, -1.0), (1.0, -1.0, -1.0))
    components = []
    for component_index in range(6):
        parity_x, parity_y, parity_z = parities[component_index]
        component = mirror_part(samples[component_index], 0, parity_z)
        component = mirror_part(component, 1, parity_x)
        component = mirror_part(component, 2, parity_y)
        if component_index < 3:
            components.append(0.3 + 2.5 * component)
        else:
            components.append(2.0 * component)
    return jnp.stack(components)


def draw_anisotropy(key, part):
    position = jnp.arange(NX, dtype=jnp.float32) / (NX - 1)
    factor = jax.random.uniform(key, (NX,), jnp.float32, 0.5, 2.0)
    return 0.5 * jnp.power(10.0, position) * factor


def draw_magnet(key, part):
    array_dims = (IMAGES, 3, NZ, NX, NY)
    position = jnp.arange(NX, dtype=jnp.float32) / (NX - 1)
    samples = jax.random.normal(key, array_dims, jnp.float32)
    growth = 0.15 * jnp.power(3.0, position)
    lateral = 0.0
    scaled = samples * growth[None, None, None, :, None]
    scaled = scaled.at[0].set(samples[0])
    wandering = jnp.cumsum(scaled, axis=0)
    image_pos = jnp.arange(IMAGES, dtype=jnp.float32) / (IMAGES - 1)
    polar_offset = 2.0 * jnp.cos(math.pi * image_pos)
    offsets = jnp.stack([jnp.zeros_like(polar_offset), jnp.full_like(polar_offset, lateral), polar_offset], axis=1)
    direction = wandering + offsets[:, :, None, None, None]
    return direction / jnp.sqrt(jnp.sum(direction * direction, axis=1, keepdims=True))


def setup_inputs(seed: int = 0) -> dict:
    key_list = jax.random.split(jax.random.key(seed), 4)
    return {
        "magnet": draw_magnet(jax.random.fold_in(key_list[3], 71), 0),
        "anisotropy": draw_anisotropy(jax.random.fold_in(key_list[3], 71), 0),
        "kernel": draw_kernel(jax.random.fold_in(key_list[3], 71), 0),
    }


exchange_strength = 0.25
chiral_strength = 0.3
spring_strength = 10.0
step_limit = 1.0
rotation_limit = 0.5
epsilon = 1e-06

def lift_axes(values):
    return values[:, None, None, None, None]

def total_cells(values):
    return lax.optimization_barrier(jnp.sum(values, axis=tuple(range(1, values.ndim))))

def project(vector, magnet):
    return vector - lax.optimization_barrier(jnp.sum(vector * magnet, axis=1, keepdims=True)) * magnet

def angle_squared(first, second):
    normal_part = jnp.cross(first, second, axis=1)
    sine_value = jnp.sqrt(lax.optimization_barrier(jnp.sum(normal_part * normal_part, axis=1)))
    cosine = lax.optimization_barrier(jnp.sum(first * second, axis=1))
    return jnp.arctan2(sine_value, cosine) ** 2

def tangent_weights(energy_total, energy_next, energy_prior):
    rise_next = energy_next - energy_total
    rise_prior = energy_total - energy_prior
    upward = (rise_next > 0) & (rise_prior > 0)
    downward = (rise_next < 0) & (rise_prior < 0)
    larger = jnp.maximum(jnp.abs(rise_next), jnp.abs(rise_prior))
    smaller = jnp.minimum(jnp.abs(rise_next), jnp.abs(rise_prior))
    toward_next = energy_next > energy_prior
    weight_next = jnp.where(upward, 1.0, jnp.where(downward, 0.0, jnp.where(toward_next, larger, smaller)))
    weight_prior = jnp.where(upward, 0.0, jnp.where(downward, 1.0, jnp.where(toward_next, smaller, larger)))
    return (weight_next, weight_prior)

def local_fields(magnet, anisotropy):
    padded = jnp.pad(magnet, ((0, 0), (0, 0), (1, 1), (1, 1), (1, 1)))
    z_plus = padded[:, :, 2:, 1:-1, 1:-1]
    z_minus = padded[:, :, :-2, 1:-1, 1:-1]
    x_plus = padded[:, :, 1:-1, 2:, 1:-1]
    x_minus = padded[:, :, 1:-1, :-2, 1:-1]
    y_plus = padded[:, :, 1:-1, 1:-1, 2:]
    y_minus = padded[:, :, 1:-1, 1:-1, :-2]
    layer_pos = lax.broadcasted_iota(jnp.int32, (NZ, NX, NY), 0)
    row_pos = lax.broadcasted_iota(jnp.int32, (NZ, NX, NY), 1)
    column_pos = lax.broadcasted_iota(jnp.int32, (NZ, NX, NY), 2)
    boundary = (layer_pos == 0).astype(jnp.float32) + (layer_pos == NZ - 1).astype(jnp.float32)
    boundary = boundary + (row_pos == 0).astype(jnp.float32) + (row_pos == NX - 1).astype(jnp.float32)
    boundary = boundary + (column_pos == 0).astype(jnp.float32) + (column_pos == NY - 1).astype(jnp.float32)
    present = 6.0 - boundary
    neighbours = x_plus + x_minus + y_plus + y_minus + z_plus + z_minus
    exchange_part = exchange_strength * (neighbours - present * magnet)
    chiral_x = chiral_strength * (x_plus[:, 2] - x_minus[:, 2])
    chiral_y = chiral_strength * (y_plus[:, 2] - y_minus[:, 2])
    chiral_z = -chiral_strength * (x_plus[:, 0] - x_minus[:, 0] + (y_plus[:, 1] - y_minus[:, 1]))
    easy_axis = 2.0 * anisotropy[:, None] * magnet[:, 2]
    return exchange_part + jnp.stack([chiral_x, chiral_y, chiral_z + easy_axis], axis=1)

def demag_one(magnet_one, kernel):
    padded = jnp.pad(magnet_one, ((0, 0), (0, NZ), (0, NX), (0, NY)))
    spectrum = jnp.fft.fftn(padded, axes=(1, 2, 3))
    spec_x = spectrum[0]
    spec_y = spectrum[1]
    spec_z = spectrum[2]
    field_x = kernel[0] * spec_x + kernel[3] * spec_y + kernel[4] * spec_z
    field_y = kernel[3] * spec_x + kernel[1] * spec_y + kernel[5] * spec_z
    field_z = kernel[4] * spec_x + kernel[5] * spec_y + kernel[2] * spec_z
    inverse = jnp.fft.ifftn(jnp.stack([field_x, field_y, field_z]), axes=(1, 2, 3))
    return -jnp.real(inverse)[:, :NZ, :NX, :NY]

def reference(magnet, anisotropy, kernel):
    cell_count = NZ * NX * NY

    def one_image(magnet_one):
        return demag_one(magnet_one, kernel)
    demag = lax.map(one_image, magnet)
    fields = local_fields(magnet, anisotropy) + demag
    energy_total = -0.5 * total_cells(magnet * fields)
    next_image = jnp.concatenate([magnet[1:], magnet[-1:]], axis=0)
    prior_image = jnp.concatenate([magnet[:1], magnet[:-1]], axis=0)
    energy_next = jnp.concatenate([energy_total[1:], energy_total[-1:]])
    energy_prior = jnp.concatenate([energy_total[:1], energy_total[:-1]])
    true_force = project(fields, magnet)
    tangent_next = project(next_image - magnet, magnet)
    tangent_prior = project(magnet - prior_image, magnet)
    distance_next = jnp.sqrt(total_cells(angle_squared(magnet, next_image)) / cell_count)
    distance_prior = jnp.sqrt(total_cells(angle_squared(magnet, prior_image)) / cell_count)
    weight_next, weight_prior = tangent_weights(energy_total, energy_next, energy_prior)
    tangent = lift_axes(weight_next) * tangent_next + lift_axes(weight_prior) * tangent_prior
    length_mean = total_cells(tangent * tangent) / cell_count
    unit_tangent = tangent / lift_axes(jnp.sqrt(length_mean + epsilon))
    parallel = total_cells(true_force * unit_tangent) / cell_count
    spring = spring_strength * (distance_next - distance_prior)
    image_index = jnp.arange(IMAGES)
    interior = (image_index > 0) & (image_index < IMAGES - 1)
    band_force = jnp.where(lift_axes(interior), true_force + lift_axes(spring - parallel) * unit_tangent, 0.0)
    largest = lax.optimization_barrier(jnp.max(jnp.sqrt(lax.optimization_barrier(jnp.sum(band_force * band_force, axis=1))), axis=(1, 2, 3)))
    move_scale = jnp.minimum(step_limit, rotation_limit / (largest + epsilon))
    stepped = magnet + lift_axes(move_scale) * band_force
    updated = stepped / jnp.sqrt(lax.optimization_barrier(jnp.sum(stepped * stepped, axis=1, keepdims=True)))
    return (updated, band_force, energy_total / cell_count)
```

```python
import math

import jax
import jax.numpy as jnp
import numpy as np
from jax import lax
from jax.experimental import pallas as pl
from jax.experimental.pallas import tpu as pltpu
from jax.sharding import PartitionSpec as P

F32 = jnp.float32
BF16 = jnp.bfloat16
MESH = pl.DeviceIdType.MESH

exchange_strength = 0.25
chiral_strength = 0.3
spring_strength = 10.0
step_limit = 1.0
rotation_limit = 0.5
epsilon = 1e-06

NZ, NROW, NY, NX = 8, 16, 256, 256
SPACE = 16
CELLS = NZ * NX * NY


def split_table(table):
    high = table.astype(np.dtype(BF16))
    low = (table - high.astype(np.float64)).astype(np.dtype(BF16))
    return high, low


def wave_table(count):
    position = 2 * np.arange(count)[:, None] - (count - 1)
    cosine = np.arange(count)[None, :]
    sine = np.where(cosine == 0, count, cosine)
    unit = 2.0 * math.pi / (4 * count)
    return np.concatenate(
        [
            np.cos((cosine * position % (4 * count)) * unit),
            np.sin((sine * position % (4 * count)) * unit),
        ],
        axis=1,
    )


def layer_wave(q, n, sine):
    angle = 2.0 * math.pi * q * (n - (NZ - 1) / 2) / (2 * NZ)
    return float(math.sin(angle) if sine else math.cos(angle))


def plane_parts(q):
    if q == 0:
        return ((0, False), (1, False))
    if q == NZ:
        return ((0, True), (1, True))
    image = 0 if q < NZ else 1
    return ((image, False), (image, True))


def split(x):
    high = x.astype(BF16)
    low = (x - high.astype(F32)).astype(BF16)
    return high, low


def mm(a, b):
    return jnp.dot(a, b, preferred_element_type=F32)


def total(x):
    return jnp.sum(jnp.sum(x, axis=0, keepdims=True), axis=1, keepdims=True)


def rows_of(values):
    row = lax.broadcasted_iota(jnp.int32, (8, 128), 0)
    tile = jnp.zeros((8, 128), F32)
    for j, v in enumerate(values):
        tile = jnp.where(row == j, v, tile)
    return tile


def step_kernel(
    m_hbm, ani_ref, k_hbm, whi_hbm, wlo_hbm, thi_hbm, tlo_hbm,
    upd_hbm, bf_hbm, en_ref,
    m, prior, nxt, halo_out, halo_in, sbuf, ybuf, zhi, zlo, spec, rhi, rlo,
    kraw, keff, uhi, ulo, fbuf, gbuf, floc, tang, out_b, out_u,
    whi, wlo, thi, tlo,
    msg_e, got_e, msg_n, got_n, msg_c, got_c, msg_d, got_d,
    in_sem, out_sem, y_s, y_r, f_s, f_r, e_s, e_r, c_s, c_r, d_s, d_r, n_s, n_r, i_s, i_r, h_s, h_r,
):
    im = lax.axis_index("image")
    me = lax.axis_index("space")
    images = lax.axis_size("image")
    hi, yy, core = me // 8, (me // 2) % 4, me % 2

    def dest(k):
        return ((hi + k // 8) % 2) * 8 + ((yy + (k // 2) % 4) % 4) * 2 + (core + k % 2) % 2

    def source(k):
        return ((hi + k // 8) % 2) * 8 + ((yy + 4 - (k // 2) % 4) % 4) * 2 + (core + k % 2) % 2

    im_next = (im + 1) % images
    im_prior = (im + images - 1) % images
    sp_next = (me + 1) % SPACE
    sp_prior = (me + SPACE - 1) % SPACE

    loads = [
        pltpu.make_async_copy(m_hbm, m, in_sem.at[0]),
        pltpu.make_async_copy(whi_hbm, whi, in_sem.at[1]),
        pltpu.make_async_copy(wlo_hbm, wlo, in_sem.at[2]),
        pltpu.make_async_copy(thi_hbm, thi, in_sem.at[3]),
        pltpu.make_async_copy(tlo_hbm, tlo, in_sem.at[4]),
        pltpu.make_async_copy(
            k_hbm.at[:, 0, pl.ds(0, NX + 8), pl.ds(0, NY + 128)], kraw, in_sem.at[5]
        ),
    ]
    for c in loads:
        c.start()

    barrier = pltpu.get_barrier_semaphore()

    def greet(k, carry):
        pl.semaphore_signal(barrier, inc=1, device_id={"space": dest(k)}, device_id_type=MESH)
        return carry

    lax.fori_loop(1, SPACE, greet, 0)
    pl.semaphore_signal(barrier, inc=1, device_id={"image": im_next}, device_id_type=MESH)
    pl.semaphore_signal(barrier, inc=1, device_id={"image": im_prior}, device_id_type=MESH)

    loads[0].wait()

    def layers_in(c, carry):
        even, odd = [], []
        for i in range(2):
            lower = [m[i, c, n] for n in range(NZ // 2)]
            upper = [m[i, c, NZ - 1 - n] for n in range(NZ // 2)]
            even.append([a + b for a, b in zip(lower, upper)])
            odd.append([a - b for a, b in zip(lower, upper)])
        for q in range(2 * NZ):
            for part, (i, sine) in enumerate(plane_parts(q)):
                terms = odd[i] if sine else even[i]
                acc = terms[0] * layer_wave(q, 0, sine)
                for n in range(1, NZ // 2):
                    acc = acc + terms[n] * layer_wave(q, n, sine)
                sbuf[q, part, c] = acc
        return carry

    lax.fori_loop(0, 3, layers_in, 0)

    for i in range(2):
        for c in range(3):
            halo_out[0, i, c] = m[i, c, :, 0, :]
            halo_out[1, i, c] = m[i, c, :, NROW - 1, :]

    pl.semaphore_wait(barrier, SPACE + 1)

    def plane_copy(k):
        return pltpu.make_async_remote_copy(
            src_ref=sbuf.at[dest(k)], dst_ref=ybuf.at[me], send_sem=y_s.at[k],
            recv_sem=y_r.at[k], device_id={"space": dest(k)}, device_id_type=MESH,
        )

    halo_copies = [
        pltpu.make_async_remote_copy(
            src_ref=halo_out.at[0], dst_ref=halo_in.at[1], send_sem=h_s.at[0],
            recv_sem=h_r.at[0], device_id={"space": sp_prior}, device_id_type=MESH,
        ),
        pltpu.make_async_remote_copy(
            src_ref=halo_out.at[1], dst_ref=halo_in.at[0], send_sem=h_s.at[1],
            recv_sem=h_r.at[1], device_id={"space": sp_next}, device_id_type=MESH,
        ),
    ]
    image_copies = [
        pltpu.make_async_remote_copy(
            src_ref=m.at[0], dst_ref=nxt, send_sem=i_s.at[0],
            recv_sem=i_r.at[0], device_id={"image": im_prior}, device_id_type=MESH,
        ),
        pltpu.make_async_remote_copy(
            src_ref=m.at[1], dst_ref=prior, send_sem=i_s.at[1],
            recv_sem=i_r.at[1], device_id={"image": im_next}, device_id_type=MESH,
        ),
    ]

    def start_plane(k, carry):
        plane_copy(SPACE - k).start()
        return carry

    lax.fori_loop(1, SPACE, start_plane, 0)
    for c in halo_copies:
        c.start()
    for c in image_copies:
        c.start()
    ybuf[pl.ds(me, 1)] = sbuf[pl.ds(me, 1)]

    loads[5].wait()
    plane_weight = jnp.where(me % NZ == 0, 1.0, 2.0) * (-4.0 / (2 * NZ * 2 * NX * 2 * NY))
    lane = lax.broadcasted_iota(jnp.int32, (64, 128), 1)

    def prepare(t, carry):
        comp, first = t // 4, pl.multiple_of((t % 4) * 64, 64)
        row = lax.broadcasted_iota(jnp.int32, (64, NY), 0) + first
        column = lax.broadcasted_iota(jnp.int32, (64, NY), 1)
        weight = plane_weight * jnp.where(row == 0, 0.5, 1.0) * jnp.where(column == 0, 0.5, 1.0)
        base = kraw[comp, pl.ds(first, 64), pl.ds(0, NY)]
        edge = kraw[comp, pl.ds(first, 64), pl.ds(NY, 128)]
        last = kraw[comp, pl.ds(NX, 8), pl.ds(0, NY)][0:1]
        last_edge = kraw[comp, pl.ds(NX, 8), pl.ds(NY, 128)][0:1]
        top = row == 0
        for bx in range(2):
            body_part = jnp.where(top, last, base) if bx else base
            edge_part = jnp.where(top[:, :128], last_edge, edge) if bx else edge
            for by in range(2):
                if by:
                    left = jnp.where(lane == 0, edge_part, body_part[:, :128])
                    value = jnp.concatenate([left, body_part[:, 128:]], axis=1)
                else:
                    value = body_part
                keff[comp, pl.ds(bx * NX + first, 64), pl.ds(by * NY, NY)] = value * weight
        return carry

    lax.fori_loop(0, 24, prepare, 0)

    for c in halo_copies:
        c.wait_recv()
    row = lax.broadcasted_iota(jnp.int32, (NROW, NY), 0)
    column = lax.broadcasted_iota(jnp.int32, (NROW, NY), 1)
    easy = jnp.zeros((NROW, NY), F32)
    for r in range(NROW):
        easy = jnp.where(row == r, 2.0 * ani_ref[r], easy)
    edges = (
        jnp.where((row == 0) & (me == 0), 1.0, 0.0)
        + jnp.where((row == NROW - 1) & (me == SPACE - 1), 1.0, 0.0)
        + jnp.where(column == 0, 1.0, 0.0)
        + jnp.where(column == NY - 1, 1.0, 0.0)
    )
    keep_first = jnp.where(me == 0, 0.0, 1.0)
    keep_last = jnp.where(me == SPACE - 1, 0.0, 1.0)

    def local_part(i):
        def layer(z, acc):
            at_bottom = z == 0
            at_top = z == NZ - 1
            present = 6.0 - edges - jnp.where(at_bottom | at_top, 1.0, 0.0)
            own, xp, xm, yp, ym, field = [], [], [], [], [], []
            for c in range(3):
                v = m[i, c, z]
                before = halo_in[0, i, c, pl.ds(z, 1), :] * keep_first
                after = halo_in[1, i, c, pl.ds(z, 1), :] * keep_last
                own.append(v)
                xp.append(jnp.where(row == NROW - 1, after, pltpu.roll(v, NROW - 1, 0)))
                xm.append(jnp.where(row == 0, before, pltpu.roll(v, 1, 0)))
                yp.append(jnp.where(column == NY - 1, 0.0, pltpu.roll(v, NY - 1, 1)))
                ym.append(jnp.where(column == 0, 0.0, pltpu.roll(v, 1, 1)))
                zp = jnp.where(at_top, 0.0, m[i, c, jnp.minimum(z + 1, NZ - 1)])
                zm = jnp.where(at_bottom, 0.0, m[i, c, jnp.maximum(z - 1, 0)])
                around = xp[c] + xm[c] + yp[c] + ym[c] + zp + zm
                field.append(exchange_strength * (around - present * v))
            field[0] = field[0] + chiral_strength * (xp[2] - xm[2])
            field[1] = field[1] + chiral_strength * (yp[2] - ym[2])
            field[2] = (
                field[2]
                - chiral_strength * ((xp[0] - xm[0]) + (yp[1] - ym[1]))
                + easy * own[2]
            )
            for c in range(3):
                floc[i, c, z] = field[c]
                acc = acc + field[c] * own[c]
            return acc

        return lax.fori_loop(0, NZ, layer, jnp.zeros((NROW, NY), F32))

    local_energy = [total(local_part(i)) for i in range(2)]

    for c in loads[1:5]:
        c.wait()

    def along_y(t, carry):
        def arrived(k, inner):
            plane_copy(k).wait_recv()
            return inner

        lax.fori_loop(jnp.maximum(2 * t, 1), 2 * t + 2, arrived, 0)
        first = ((hi + t // 4) % 2) * 8 + ((yy + 4 - t % 4) % 4) * 2
        data = ybuf[pl.ds(first, 2)].reshape(2 * 6 * NROW, NY)
        high, low = split(data)
        out = mm(high, whi[...]) + mm(high, wlo[...]) + mm(low, whi[...])
        ohigh, olow = split(out)
        ohigh = ohigh.reshape(2, 6, NROW, 2 * NY)
        olow = olow.reshape(2, 6, NROW, 2 * NY)
        for u in range(2):
            at = pl.multiple_of((first + u) * NROW, NROW)
            for j in range(6):
                zhi[j, pl.ds(at, NROW), :] = ohigh[u, j]
                zlo[j, pl.ds(at, NROW), :] = olow[u, j]
        return carry

    lax.fori_loop(0, 8, along_y, 0)

    def along_x(j, carry):
        for r in range(2):
            for n in range(2):
                rs, ns = pl.ds(r * NX, NX), pl.ds(n * NY, NY)
                zh, zl = zhi[j, :, ns], zlo[j, :, ns]
                spec[j, rs, ns] = mm(thi[rs, :], zh) + mm(tlo[rs, :], zh) + mm(thi[rs, :], zl)
        return carry

    lax.fori_loop(0, 6, along_x, 0)

    def respond(t, acc):
        r0 = pl.multiple_of((t // 2) * 16, 16)
        l0 = pl.multiple_of((t % 2) * 128, 128)
        acc = list(acc)
        for bx in range(2):
            for by in range(2):
                def at(bx_, by_):
                    return (pl.ds(bx_ * NX + r0, 16), pl.ds(by_ * NY + l0, 128))

                here = at(bx, by)
                k = [keff[(comp, *here)] for comp in range(6)]
                for a in range(2):
                    v = [spec[(3 * a + c, *here)] for c in range(3)]
                    b = 1 - a
                    xy = [spec[(3 * a + c, *at(1 - bx, 1 - by))] for c in (0, 1)]
                    xz = [spec[(3 * b + c, *at(1 - bx, by))] for c in (0, 2)]
                    yz = [spec[(3 * b + c, *at(bx, 1 - by))] for c in (1, 2)]
                    sxy = -1.0 if bx == by else 1.0
                    sxz = -1.0 if a == bx else 1.0
                    syz = -1.0 if a == by else 1.0

                    def plus(x, s, y):
                        return x + y if s > 0 else x - y

                    fx = plus(plus(k[0] * v[0], sxy, k[3] * xy[1]), sxz, k[4] * xz[1])
                    fy = plus(plus(k[1] * v[1], sxy, k[3] * xy[0]), syz, k[5] * yz[1])
                    fz = plus(plus(k[2] * v[2], sxz, k[4] * xz[0]), syz, k[5] * yz[0])
                    acc[a] = acc[a] + (fx * v[0] + fy * v[1] + fz * v[2])
                    for c, f in enumerate((fx, fy, fz)):
                        high, low = split(f)
                        rhi[(3 * a + c, *here)] = high
                        rlo[(3 * a + c, *here)] = low
        return tuple(acc)

    zero = jnp.zeros((16, 128), F32)
    part_a, part_b = (total(x) for x in lax.fori_loop(0, 32, respond, (zero, zero)))
    none = jnp.zeros((1, 1), F32)
    first_share = jnp.where(me <= NZ, part_a, none) + jnp.where(
        (me >= 1) & (me < NZ), part_b, none
    )
    second_share = jnp.where(me > NZ, part_a, none) + jnp.where(
        (me == 0) | (me >= NZ), part_b, none
    )

    def small_round(msg, got, s_sem, r_sem):
        def copy(k):
            return pltpu.make_async_remote_copy(
                src_ref=msg, dst_ref=got.at[me], send_sem=s_sem.at[k],
                recv_sem=r_sem.at[k], device_id={"space": dest(k)}, device_id_type=MESH,
            )

        def start():
            lax.fori_loop(1, SPACE, lambda k, x: (copy(k).start(), x)[1], 0)

        def finish():
            lax.fori_loop(1, SPACE, lambda k, x: (copy(k).wait_recv(), x)[1], 0)

        def drain():
            lax.fori_loop(1, SPACE, lambda k, x: (copy(k).wait_send(), x)[1], 0)

        return start, finish, drain

    def send_round(rnd, msg, got, tile):
        msg[...] = tile
        got[me] = tile
        rnd[0]()

    def sum_round(got):
        acc = got[0]
        for s in range(1, SPACE):
            acc = acc + got[s]
        return acc

    round_e = small_round(msg_e, got_e, e_s, e_r)
    round_c = small_round(msg_c, got_c, c_s, c_r)
    round_d = small_round(msg_d, got_d, d_s, d_r)
    send_round(
        round_e, msg_e, got_e,
        rows_of([local_energy[0] + first_share, local_energy[1] + second_share]),
    )

    def back_x(j, carry):
        for n in range(2):
            ns = pl.ds(n * NY, NY)
            rh, rl = rhi[j, :, ns], rlo[j, :, ns]
            u = mm(whi[...], rh) + mm(wlo[...], rh) + mm(whi[...], rl)
            high, low = split(u)
            uhi[j, :, ns] = high
            ulo[j, :, ns] = low
        return carry

    lax.fori_loop(0, 6, back_x, 0)

    round_e[1]()
    energy = -0.5 * sum_round(got_e)
    msg_n[...] = energy
    energy_copies = [
        pltpu.make_async_remote_copy(
            src_ref=msg_n, dst_ref=got_n.at[1], send_sem=n_s.at[0],
            recv_sem=n_r.at[0], device_id={"image": im_prior}, device_id_type=MESH,
        ),
        pltpu.make_async_remote_copy(
            src_ref=msg_n, dst_ref=got_n.at[0], send_sem=n_s.at[1],
            recv_sem=n_r.at[1], device_id={"image": im_next}, device_id_type=MESH,
        ),
    ]
    for c in energy_copies:
        c.start()

    def back_y(j, carry):
        uh, ul = uhi[j], ulo[j]
        f = mm(uh, thi[...]) + mm(uh, tlo[...]) + mm(ul, thi[...])
        fbuf[:, j] = f.reshape(SPACE, NROW, NY)
        return carry

    lax.fori_loop(0, 6, back_y, 0)

    def field_copy(k):
        return pltpu.make_async_remote_copy(
            src_ref=fbuf.at[dest(k)], dst_ref=gbuf.at[me], send_sem=f_s.at[k],
            recv_sem=f_r.at[k], device_id={"space": dest(k)}, device_id_type=MESH,
        )

    lax.fori_loop(1, SPACE, lambda k, x: (field_copy(SPACE - k).start(), x)[1], 0)
    gbuf[pl.ds(me, 1)] = fbuf[pl.ds(me, 1)]

    en_ref[0] = jnp.max(energy[0:1]) / CELLS
    en_ref[1] = jnp.max(energy[1:2]) / CELLS

    for c in image_copies:
        c.wait_recv()

    def angle_squared(a, b):
        n0 = a[1] * b[2] - a[2] * b[1]
        n1 = a[2] * b[0] - a[0] * b[2]
        n2 = a[0] * b[1] - a[1] * b[0]
        sine = jnp.sqrt(n0 * n0 + n1 * n1 + n2 * n2)
        cosine = a[0] * b[0] + a[1] * b[1] + a[2] * b[2]
        angle = jnp.arctan2(sine, cosine)
        return angle * angle

    def distances(z, acc):
        p = [prior[c, z] for c in range(3)]
        a = [m[0, c, z] for c in range(3)]
        b = [m[1, c, z] for c in range(3)]
        n = [nxt[c, z] for c in range(3)]
        return (
            acc[0] + angle_squared(a, p),
            acc[1] + angle_squared(a, b),
            acc[2] + angle_squared(b, n),
        )

    flat = jnp.zeros((NROW, NY), F32)
    spans = [total(x) for x in lax.fori_loop(0, NZ, distances, (flat, flat, flat))]

    for c in energy_copies:
        c.wait_recv()
    e_prior, e_own, e_next = got_n[0][1:2, 0:1], energy, got_n[1][0:1, 0:1]
    line = [e_prior, e_own[0:1, 0:1], e_own[1:2, 0:1], e_next]
    lengths = []
    for i in range(2):
        rise_next = line[i + 2] - line[i + 1]
        rise_prior = line[i + 1] - line[i]
        upward = (rise_next > 0) & (rise_prior > 0)
        downward = (rise_next < 0) & (rise_prior < 0)
        larger = jnp.maximum(jnp.abs(rise_next), jnp.abs(rise_prior))
        smaller = jnp.minimum(jnp.abs(rise_next), jnp.abs(rise_prior))
        toward_next = line[i + 2] > line[i]
        one, nil = jnp.ones((1, 1), F32), jnp.zeros((1, 1), F32)
        w_next = jnp.where(
            upward, one, jnp.where(downward, nil, jnp.where(toward_next, larger, smaller))
        )
        w_prior = jnp.where(
            upward, nil, jnp.where(downward, one, jnp.where(toward_next, smaller, larger))
        )
        w_next = jnp.broadcast_to(w_next, (NROW, NY))
        w_prior = jnp.broadcast_to(w_prior, (NROW, NY))

        def tangent(z, acc, i=i, w_next=w_next, w_prior=w_prior):
            own = [m[i, c, z] for c in range(3)]
            ahead = [m[1, c, z] if i == 0 else nxt[c, z] for c in range(3)]
            behind = [prior[c, z] if i == 0 else m[0, c, z] for c in range(3)]
            v = [
                w_next * (ahead[c] - own[c]) + w_prior * (own[c] - behind[c]) for c in range(3)
            ]
            along = v[0] * own[0] + v[1] * own[1] + v[2] * own[2]
            for c in range(3):
                t = v[c] - along * own[c]
                tang[i, c, z] = t
                acc = acc + t * t
            return acc

        lengths.append(total(lax.fori_loop(0, NZ, tangent, flat)))

    lax.fori_loop(1, SPACE, lambda k, x: (field_copy(k).wait_recv(), x)[1], 0)

    def layers_out(c, carry):
        for i in range(2):
            even = [None] * (NZ // 2)
            odd = [None] * (NZ // 2)
            for q in range(2 * NZ):
                for part, (image, sine) in enumerate(plane_parts(q)):
                    if image != i:
                        continue
                    v = gbuf[q, 3 * part + c]
                    acc = odd if sine else even
                    for n in range(NZ // 2):
                        term = v * layer_wave(q, n, sine)
                        acc[n] = term if acc[n] is None else acc[n] + term
            for n in range(NZ // 2):
                floc[i, c, n] = floc[i, c, n] + (even[n] + odd[n])
                floc[i, c, NZ - 1 - n] = floc[i, c, NZ - 1 - n] + (even[n] - odd[n])
        return carry

    lax.fori_loop(0, 3, layers_out, 0)

    drives = []
    for i in range(2):
        def force(z, acc, i=i):
            own = [m[i, c, z] for c in range(3)]
            f = [floc[i, c, z] for c in range(3)]
            along = f[0] * own[0] + f[1] * own[1] + f[2] * own[2]
            for c in range(3):
                t = f[c] - along * own[c]
                floc[i, c, z] = t
                acc = acc + t * tang[i, c, z]
            return acc

        drives.append(total(lax.fori_loop(0, NZ, force, flat)))

    send_round(round_c, msg_c, got_c, rows_of(lengths + drives + spans))
    round_c[1]()
    sums = sum_round(got_c)
    dist = [jnp.sqrt(sums[4 + j : 5 + j, 0:1] / CELLS) for j in range(3)]
    tops = []
    for i in range(2):
        scale = jnp.sqrt(sums[i : i + 1, 0:1] / CELLS + epsilon)
        parallel = sums[2 + i : 3 + i, 0:1] / (CELLS * scale)
        spring = spring_strength * (dist[i + 1] - dist[i])
        index = 2 * im + i
        interior = (index > 0) & (index < 2 * images - 1)
        coef = jnp.broadcast_to((spring - parallel) / scale, (NROW, NY))
        inner = jnp.where(interior, 1, 0)

        def band(z, acc, i=i, coef=coef, inner=inner):
            size = None
            for c in range(3):
                b = floc[i, c, z] + coef * tang[i, c, z]
                b = jnp.where(inner > 0, b, 0.0)
                out_b[i, c, z] = b
                size = b * b if size is None else size + b * b
            return jnp.maximum(acc, size)

        top = lax.fori_loop(0, NZ, band, flat)
        tops.append(jnp.max(jnp.max(top, axis=0, keepdims=True), axis=1, keepdims=True))

    send_round(round_d, msg_d, got_d, rows_of(tops))
    store_b = pltpu.make_async_copy(out_b, bf_hbm, out_sem.at[0])
    store_b.start()
    round_d[1]()
    largest = got_d[0]
    for s in range(1, SPACE):
        largest = jnp.maximum(largest, got_d[s])
    largest = jnp.sqrt(largest)
    for i in range(2):
        move = jnp.minimum(step_limit, rotation_limit / (largest[i : i + 1, 0:1] + epsilon))
        move = jnp.broadcast_to(move, (NROW, NY))

        def advance(z, carry, i=i, move=move):
            s = [m[i, c, z] + move * out_b[i, c, z] for c in range(3)]
            length = jnp.sqrt(s[0] * s[0] + s[1] * s[1] + s[2] * s[2])
            for c in range(3):
                out_u[i, c, z] = s[c] / length
            return carry

        lax.fori_loop(0, NZ, advance, 0)
    store_u = pltpu.make_async_copy(out_u, upd_hbm, out_sem.at[1])
    store_u.start()

    lax.fori_loop(1, SPACE, lambda k, x: (plane_copy(k).wait_send(), x)[1], 0)
    lax.fori_loop(1, SPACE, lambda k, x: (field_copy(k).wait_send(), x)[1], 0)
    for rnd in (round_e, round_c, round_d):
        rnd[2]()
    for c in halo_copies + image_copies + energy_copies:
        c.wait_send()
    store_b.wait()
    store_u.wait()


def body(magnet, anisotropy, kernel):
    table = wave_table(NX)
    w_high, w_low = split_table(table)
    t_high, t_low = split_table(np.ascontiguousarray(table.T))
    slab = (2, 3, NZ, NROW, NY)
    vm = pltpu.VMEM
    dma = pltpu.SemaphoreType.DMA
    tile = (8, 128)
    scratch = [
        vm(slab, F32), vm(slab[1:], F32), vm(slab[1:], F32),
        vm((2, 2, 3, NZ, NY), F32), vm((2, 2, 3, NZ, NY), F32),
        vm((SPACE, 2, 3, NROW, NY), F32), vm((SPACE, 2, 3, NROW, NY), F32),
        vm((6, NX, 2 * NY), BF16), vm((6, NX, 2 * NY), BF16),
        vm((6, 2 * NX, 2 * NY), F32),
        vm((6, 2 * NX, 2 * NY), BF16), vm((6, 2 * NX, 2 * NY), BF16),
        vm((6, NX + 8, NY + 128), F32), vm((6, 2 * NX, 2 * NY), F32),
        vm((6, NX, 2 * NY), BF16), vm((6, NX, 2 * NY), BF16),
        vm((SPACE, 6, NROW, NY), F32), vm((SPACE, 6, NROW, NY), F32),
        vm(slab, F32), vm(slab, F32), vm(slab, F32), vm(slab, F32),
        vm((NX, 2 * NY), BF16), vm((NX, 2 * NY), BF16),
        vm((2 * NX, NY), BF16), vm((2 * NX, NY), BF16),
        vm(tile, F32), vm((SPACE, *tile), F32),
        vm(tile, F32), vm((2, *tile), F32),
        vm(tile, F32), vm((SPACE, *tile), F32),
        vm(tile, F32), vm((SPACE, *tile), F32),
        dma((6,)), dma((2,)),
        dma((SPACE,)), dma((SPACE,)), dma((SPACE,)), dma((SPACE,)),
        dma((SPACE,)), dma((SPACE,)), dma((SPACE,)), dma((SPACE,)),
        dma((SPACE,)), dma((SPACE,)),
        dma((2,)), dma((2,)), dma((2,)), dma((2,)), dma((2,)), dma((2,)),
    ]
    anyspace = pl.BlockSpec(memory_space=pl.ANY)
    return pl.pallas_call(
        step_kernel,
        out_shape=(
            jax.ShapeDtypeStruct(slab, F32),
            jax.ShapeDtypeStruct(slab, F32),
            jax.ShapeDtypeStruct((2,), F32),
        ),
        in_specs=[anyspace, pl.BlockSpec(memory_space=pltpu.SMEM)] + [anyspace] * 5,
        out_specs=(anyspace, anyspace, pl.BlockSpec(memory_space=pltpu.SMEM)),
        scratch_shapes=scratch,
        compiler_params=pltpu.CompilerParams(
            collective_id=0, has_side_effects=True, vmem_limit_bytes=60 * 2**20
        ),
        name="band_step",
    )(
        magnet, anisotropy, kernel,
        jnp.asarray(w_high), jnp.asarray(w_low), jnp.asarray(t_high), jnp.asarray(t_low),
    )


def solution(mesh):
    in_specs = (P("image", None, None, "space", None), P("space"), P(None, "space", None, None))
    out_specs = (
        P("image", None, None, "space", None),
        P("image", None, None, "space", None),
        P("image"),
    )
    return jax.shard_map(body, mesh=mesh, in_specs=in_specs, out_specs=out_specs, check_vma=False)
```

```python
import math

import jax
import jax.numpy as jnp
import numpy as np
from jax import lax
from jax.experimental import pallas as pl
from jax.experimental.pallas import tpu as pltpu
from jax.sharding import PartitionSpec as P

F32 = jnp.float32
BF16 = jnp.bfloat16
MESH = pl.DeviceIdType.MESH

exchange_strength = 0.25
chiral_strength = 0.3
spring_strength = 10.0
step_limit = 1.0
rotation_limit = 0.5
epsilon = 1e-06

NZ, NROW, NY, NX = 8, 16, 256, 256
SPACE = 16
CELLS = NZ * NX * NY
STEP_VMEM = 53200 * 1024


def split_table(table):
    high = table.astype(np.dtype(BF16))
    low = (table - high.astype(np.float64)).astype(np.dtype(BF16))
    return high, low


def wave_table(count):
    position = 2 * np.arange(count)[:, None] - (count - 1)
    cosine = np.arange(count)[None, :]
    sine = np.where(cosine == 0, count, cosine)
    unit = 2.0 * math.pi / (4 * count)
    return np.concatenate(
        [
            np.cos((cosine * position % (4 * count)) * unit),
            np.sin((sine * position % (4 * count)) * unit),
        ],
        axis=1,
    )


def layer_wave(q, n, sine):
    angle = 2.0 * math.pi * q * (n - (NZ - 1) / 2) / (2 * NZ)
    return float(math.sin(angle) if sine else math.cos(angle))


def split(x):
    high = x.astype(BF16)
    low = (x - high.astype(F32)).astype(BF16)
    return high, low


def mm(a, b):
    return jnp.dot(a, b, preferred_element_type=F32)


def total(x):
    return jnp.sum(jnp.sum(x, axis=0, keepdims=True), axis=1, keepdims=True)


def line_of(values):
    lane = lax.broadcasted_iota(jnp.int32, (1, 128), 1)
    line = jnp.zeros((1, 128), F32)
    for j, v in enumerate(values):
        line = jnp.where(lane == j, v, line)
    return line


def step_kernel(
    m_hbm, ani_hbm, k_hbm, tab_hbm,
    m, out_b, tile_x,
    prior, nxt, halo_out, halo_in, pbuf, xbuf, sbuf, ybuf, zhi, zlo, spec, rhi, rlo,
    kraw, keff, uhi, ulo, fbuf, gbuf, obuf, rbuf, hbuf, floc, tang,
    wtab, ttab, ani_ref,
    msg_e, got_e, msg_c, got_c, msg_d, got_d,
    in_sem, p_s, p_r, x_s, x_r, y_s, y_r, f_s, f_r, g_s, g_r, o_s, o_r,
    e_s, e_r, n_s, n_r, c_s, c_r, d_s, d_r, i_s, i_r, h_s, h_r,
):
    im = lax.axis_index("image")
    me = lax.axis_index("space")
    images = lax.axis_size("image")
    hi, spot = me // NZ, me % NZ
    partner = (1 - hi) * NZ + spot
    special = spot == 0
    start_part = hi

    def dest(k):
        return (me + k) % SPACE

    def near(k):
        return hi * NZ + (spot + k) % NZ

    def each(lo, up, do):
        lax.fori_loop(lo, up, lambda k, x: (do(k), x)[1], 0)

    def remote(src, dst, send, recv, device):
        return pltpu.make_async_remote_copy(
            src_ref=src, dst_ref=dst, send_sem=send, recv_sem=recv,
            device_id={"space": device}, device_id_type=MESH,
        )

    def wait_bytes(ref, sem):
        pltpu.make_async_copy(ref, ref, sem).wait()

    def plane_sides(h):
        rows = [(0, h, h == 1, NZ * h)]
        for t in range(1, NZ):
            rows += [(t, 0, False, NZ * h + t), (t, 1, True, NZ * h + t)]
        return rows

    def layer_sums(lines):
        half = NZ // 2
        even = [lines[n] + lines[NZ - 1 - n] for n in range(half)]
        odd = [lines[n] - lines[NZ - 1 - n] for n in range(half)]
        return even, odd

    def layer_dot(terms, q, sine):
        acc = terms[0] * layer_wave(q, 0, sine)
        for n in range(1, NZ // 2):
            acc = acc + terms[n] * layer_wave(q, n, sine)
        return acc

    has_next, has_prior = im < images - 1, im > 0
    im_next = jnp.minimum(im + 1, images - 1)
    im_prior = jnp.maximum(im - 1, 0)
    sp_next = jnp.minimum(me + 1, SPACE - 1)
    sp_prior = jnp.maximum(me - 1, 0)

    loads = [
        pltpu.make_async_copy(tab_hbm.at[pl.ds(0, 2 * NX)], wtab, in_sem.at[0]),
        pltpu.make_async_copy(
            tab_hbm.at[pl.ds(2 * NX, 2 * NX), pl.ds(0, NY)], ttab.at[0], in_sem.at[1]
        ),
        pltpu.make_async_copy(
            tab_hbm.at[pl.ds(2 * NX, 2 * NX), pl.ds(NY, NY)], ttab.at[1], in_sem.at[2]
        ),
        pltpu.make_async_copy(ani_hbm, ani_ref, in_sem.at[3]),
        pltpu.make_async_copy(
            k_hbm.at[:, 0, pl.ds(0, NX + 8), pl.ds(0, NY + 128)], kraw, in_sem.at[4]
        ),
    ]
    load_m = pltpu.make_async_copy(m_hbm, m, in_sem.at[5])
    load_m.start()
    for c in loads:
        c.start()
    whi, wlo = wtab.at[pl.ds(0, NX)], wtab.at[pl.ds(NX, NX)]
    thi, tlo = ttab.at[0], ttab.at[1]

    barrier = pltpu.get_barrier_semaphore()

    def greet(k, carry):
        pl.semaphore_signal(barrier, inc=1, device_id={"space": dest(k)}, device_id_type=MESH)
        return carry

    lax.fori_loop(1, SPACE, greet, 0)

    def at_images(do):
        for present, other, slot in ((has_next, im_next, 0), (has_prior, im_prior, 1)):
            @pl.when(present)
            def _(other=other, slot=slot):
                do(other, slot)

    at_images(
        lambda other, slot: each(
            0, SPACE,
            lambda k: pl.semaphore_signal(
                barrier, inc=1, device_id={"image": other, "space": k}, device_id_type=MESH
            ),
        )
    )
    greeted = SPACE - 1 + SPACE * (jnp.minimum(im, 1) + jnp.minimum(images - 1 - im, 1))

    load_m.wait()
    def layers_in(u, c, line):
        for h in range(2):
            @pl.when(hi == h)
            def _(h=h):
                even, odd = layer_sums([line(h, n) for n in range(NZ)])
                for t, part, sine, q in plane_sides(h):
                    sbuf[u, t, 2 * c + part] = layer_dot(odd if sine else even, q, sine)

    def own_layers(c):
        layers_in(0, c, lambda h, n: m[h, c, n])
        even, _ = layer_sums([m[1, c, n] for n in range(NZ)])
        _, odd = layer_sums([m[0, c, n] for n in range(NZ)])
        xbuf[0, c] = layer_dot(even, 0, False)
        xbuf[1, c] = layer_dot(odd, NZ, True)

    each(0, 3, own_layers)

    for i in range(2):
        for c in range(3):
            halo_out[0, i, c] = m[i, c, :, 0, :]
            halo_out[1, i, c] = m[i, c, :, NROW - 1, :]

    pl.semaphore_wait(barrier, greeted)

    def partner_copy(c):
        return remote(m.at[1 - hi, c], pbuf.at[c], p_s.at[c], p_r.at[c], partner)

    def plane_copy(u, j, k):
        to = near(k)
        slab = me if u == 0 else partner
        return remote(
            sbuf.at[u, to % NZ, j], ybuf.at[j, slab], y_s.at[k], y_r.at[j], to
        )

    def extra_copy(t, c):
        return remote(
            xbuf.at[t, c], ybuf.at[2 * c + 1 - t, me], x_s.at[t], x_r.at[c], t * NZ
        )

    def send_planes(u, first, last):
        def one(j):
            def to(k):
                @pl.when((near(k) % NZ != 0) | (j % 2 == start_part))
                def _():
                    plane_copy(u, j, k).start()

            each(1, NZ, to)

            @pl.when(jnp.logical_not(special) | (j % 2 == start_part))
            def _():
                slab = me if u == 0 else partner
                ybuf[j, pl.ds(slab, 1)] = sbuf[u, spot, pl.ds(j, 1)]

        each(first, last, one)

    def halo_copy(side):
        return remote(
            halo_out.at[side], halo_in.at[1 - side], h_s.at[side], h_r.at[side],
            (sp_prior, sp_next)[side],
        )

    def at_slabs(do):
        for side, present in ((0, me > 0), (1, me < SPACE - 1)):
            @pl.when(present)
            def _(side=side):
                do(side)

    def image_copy(other, slot):
        return pltpu.make_async_remote_copy(
            src_ref=m.at[1 - slot], dst_ref=(prior, nxt)[slot], send_sem=i_s.at[slot],
            recv_sem=i_r.at[slot], device_id={"image": other}, device_id_type=MESH,
        )

    at_slabs(lambda side: halo_copy(side).start())
    for t in range(2):
        @pl.when(me != t * NZ)
        def _(t=t):
            each(0, 3, lambda c: extra_copy(t, c).start())

        @pl.when(me == t * NZ)
        def _(t=t):
            for c in range(3):
                ybuf[2 * c + 1 - t, pl.ds(me, 1)] = xbuf[t, pl.ds(c, 1)]

    each(0, 3, lambda c: partner_copy(c).start())
    send_planes(0, 0, 6)

    loads[4].wait()
    plane_weight = jnp.where(me % NZ == 0, 1.0, 2.0) * (-4.0 / (2 * NZ * 2 * NX * 2 * NY))
    lane = lax.broadcasted_iota(jnp.int32, (64, 128), 1)

    def prepare(t, carry):
        comp, first = t // 4, pl.multiple_of((t % 4) * 64, 64)
        row = lax.broadcasted_iota(jnp.int32, (64, NY), 0) + first
        column = lax.broadcasted_iota(jnp.int32, (64, NY), 1)
        weight = plane_weight * jnp.where(row == 0, 0.5, 1.0) * jnp.where(column == 0, 0.5, 1.0)
        base = kraw[comp, pl.ds(first, 64), pl.ds(0, NY)]
        edge = kraw[comp, pl.ds(first, 64), pl.ds(NY, 128)]
        last = kraw[comp, pl.ds(NX, 8), pl.ds(0, NY)][0:1]
        last_edge = kraw[comp, pl.ds(NX, 8), pl.ds(NY, 128)][0:1]
        top = row == 0
        for bx in range(2):
            body_part = jnp.where(top, last, base) if bx else base
            edge_part = jnp.where(top[:, :128], last_edge, edge) if bx else edge
            for by in range(2):
                if by:
                    left = jnp.where(lane == 0, edge_part, body_part[:, :128])
                    value = jnp.concatenate([left, body_part[:, 128:]], axis=1)
                else:
                    value = body_part
                keff[comp, pl.ds(bx * NX + first, 64), pl.ds(by * NY, NY)] = value * weight
        return carry

    lax.fori_loop(0, 24, prepare, 0)

    def partner_layers(c):
        partner_copy(c).wait_recv()
        layers_in(1, c, lambda h, n: pbuf[c, n])
        send_planes(1, 2 * c, 2 * c + 2)

    partner_layers(0)

    @pl.when(me < SPACE - 1)
    def _():
        halo_copy(0).wait_recv()

    @pl.when(me > 0)
    def _():
        halo_copy(1).wait_recv()

    row = lax.broadcasted_iota(jnp.int32, (NROW, NY), 0)
    column = lax.broadcasted_iota(jnp.int32, (NROW, NY), 1)
    loads[3].wait()
    easy = jnp.zeros((NROW, NY), F32)
    for r in range(NROW):
        easy = jnp.where(row == r, 2.0 * ani_ref[r], easy)
    edges = (
        jnp.where((row == 0) & (me == 0), 1.0, 0.0)
        + jnp.where((row == NROW - 1) & (me == SPACE - 1), 1.0, 0.0)
        + jnp.where(column == 0, 1.0, 0.0)
        + jnp.where(column == NY - 1, 1.0, 0.0)
    )

    def local_part(i):
        def layer(z, acc):
            at_bottom = z == 0
            at_top = z == NZ - 1
            present = 6.0 - edges - jnp.where(at_bottom | at_top, 1.0, 0.0)
            own, xp, xm, yp, ym, field = [], [], [], [], [], []
            for c in range(3):
                v = m[i, c, z]
                before = jnp.where(me == 0, 0.0, halo_in[0, i, c, pl.ds(z, 1), :])
                after = jnp.where(me == SPACE - 1, 0.0, halo_in[1, i, c, pl.ds(z, 1), :])
                own.append(v)
                xp.append(jnp.where(row == NROW - 1, after, pltpu.roll(v, NROW - 1, 0)))
                xm.append(jnp.where(row == 0, before, pltpu.roll(v, 1, 0)))
                yp.append(jnp.where(column == NY - 1, 0.0, pltpu.roll(v, NY - 1, 1)))
                ym.append(jnp.where(column == 0, 0.0, pltpu.roll(v, 1, 1)))
                zp = jnp.where(at_top, 0.0, m[i, c, jnp.minimum(z + 1, NZ - 1)])
                zm = jnp.where(at_bottom, 0.0, m[i, c, jnp.maximum(z - 1, 0)])
                around = xp[c] + xm[c] + yp[c] + ym[c] + zp + zm
                field.append(exchange_strength * (around - present * v))
            field[0] = field[0] + chiral_strength * (xp[2] - xm[2])
            field[1] = field[1] + chiral_strength * (yp[2] - ym[2])
            field[2] = (
                field[2]
                - chiral_strength * ((xp[0] - xm[0]) + (yp[1] - ym[1]))
                + easy * own[2]
            )
            for c in range(3):
                floc[i, c, z] = field[c]
                acc = acc + field[c] * own[c]
            return acc

        return lax.fori_loop(0, NZ, layer, jnp.zeros((NROW, NY), F32))

    local_energy = [total(local_part(0))]
    partner_layers(1)
    local_energy.append(total(local_part(1)))
    partner_layers(2)
    at_images(lambda other, slot: image_copy(other, slot).start())

    for c in loads[0:3]:
        c.wait()

    def forward(j, carry):
        regular = jnp.logical_not(special) | (j % 2 == start_part)

        @pl.when(regular)
        def _():
            wait_bytes(ybuf.at[j, pl.ds(0, SPACE - 2)], y_r.at[j])

        @pl.when(jnp.logical_not(regular))
        def _():
            wait_bytes(ybuf.at[j, pl.ds(0, SPACE - 1)], x_r.at[j // 2])

        high, low = split(ybuf[j].reshape(NX, NY))
        for n in range(2):
            ns = pl.ds(n * NY, NY)
            out = mm(high, whi[:, ns]) + mm(high, wlo[:, ns]) + mm(low, whi[:, ns])
            zhi[:, ns], zlo[:, ns] = split(out)
        for r in range(2):
            for n in range(2):
                rs, ns = pl.ds(r * NX, NX), pl.ds(n * NY, NY)
                zh, zl = zhi[:, ns], zlo[:, ns]
                spec[j, rs, ns] = mm(thi[rs, :], zh) + mm(tlo[rs, :], zh) + mm(thi[rs, :], zl)
        return carry

    lax.fori_loop(0, 6, forward, 0)

    def respond(t, acc):
        r0 = pl.multiple_of((t // 2) * 16, 16)
        l0 = pl.multiple_of((t % 2) * 128, 128)
        acc = list(acc)
        for bx in range(2):
            for by in range(2):
                def at(bx_, by_):
                    return (pl.ds(bx_ * NX + r0, 16), pl.ds(by_ * NY + l0, 128))

                here = at(bx, by)
                k = [keff[(comp, *here)] for comp in range(6)]
                for a in range(2):
                    v = [spec[(2 * c + a, *here)] for c in range(3)]
                    b = 1 - a
                    xy = [spec[(2 * c + a, *at(1 - bx, 1 - by))] for c in (0, 1)]
                    xz = [spec[(2 * c + b, *at(1 - bx, by))] for c in (0, 2)]
                    yz = [spec[(2 * c + b, *at(bx, 1 - by))] for c in (1, 2)]
                    sxy = -1.0 if bx == by else 1.0
                    sxz = -1.0 if a == bx else 1.0
                    syz = -1.0 if a == by else 1.0

                    def plus(x, s, y):
                        return x + y if s > 0 else x - y

                    fx = plus(plus(k[0] * v[0], sxy, k[3] * xy[1]), sxz, k[4] * xz[1])
                    fy = plus(plus(k[1] * v[1], sxy, k[3] * xy[0]), syz, k[5] * yz[1])
                    fz = plus(plus(k[2] * v[2], sxz, k[4] * xz[0]), syz, k[5] * yz[0])
                    acc[a] = acc[a] + (fx * v[0] + fy * v[1] + fz * v[2])
                    for c, f in enumerate((fx, fy, fz)):
                        high, low = split(f)
                        rhi[(2 * c + a, *here)] = high
                        rlo[(2 * c + a, *here)] = low
        return tuple(acc)

    zero = jnp.zeros((16, 128), F32)
    part_a, part_b = (total(x) for x in lax.fori_loop(0, 32, respond, (zero, zero)))
    none = jnp.zeros((1, 1), F32)
    first_share = jnp.where(me <= NZ, part_a, none) + jnp.where(
        (me >= 1) & (me < NZ), part_b, none
    )
    second_share = jnp.where(me > NZ, part_a, none) + jnp.where(
        (me == 0) | (me >= NZ), part_b, none
    )

    def small_round(msg, got, s_sem, r_sem):
        def copy(k):
            return pltpu.make_async_remote_copy(
                src_ref=msg, dst_ref=got.at[me], send_sem=s_sem,
                recv_sem=r_sem, device_id={"space": dest(k)}, device_id_type=MESH,
            )

        part = got.at[pl.ds(0, SPACE - 1)]

        def start():
            lax.fori_loop(1, SPACE, lambda k, x: (copy(k).start(), x)[1], 0)

        def finish():
            pltpu.make_async_copy(part, part, r_sem).wait()

        def drain():
            pltpu.make_async_copy(part, part, s_sem).wait()

        return start, finish, drain

    def send_round(rnd, msg, got, tile):
        msg[...] = tile
        got[me] = tile
        rnd[0]()

    def sum_round(got):
        acc = got[0]
        for s in range(1, SPACE):
            acc = acc + got[s]
        return acc

    round_c = small_round(msg_c, got_c, c_s, c_r)
    round_d = small_round(msg_d, got_d, d_s, d_r)

    def energy_copy(k):
        return pltpu.make_async_remote_copy(
            src_ref=msg_e, dst_ref=got_e.at[1, me], send_sem=e_s,
            recv_sem=e_r, device_id={"space": dest(k)}, device_id_type=MESH,
        )

    def image_energy_copy(other, slot, k):
        return pltpu.make_async_remote_copy(
            src_ref=msg_e, dst_ref=got_e.at[2 * slot, me], send_sem=n_s.at[slot],
            recv_sem=n_r.at[slot], device_id={"image": other, "space": k},
            device_id_type=MESH,
        )

    def field_copy(u, j, k):
        to = near(k)
        slab = to if u == 0 else (1 - hi) * NZ + to % NZ
        return remote(
            fbuf.at[j, slab], gbuf.at[u, j, spot], f_s.at[k], f_r.at[u, j], to
        )

    def return_copy(c, k):
        part = 1 - hi
        to = dest(k)
        return remote(
            fbuf.at[2 * c + part, to], hbuf.at[1 - hi, c], g_s, g_r.at[1 - hi], to
        )

    def send_fields(u, j):
        @pl.when(jnp.logical_not(special) | (j % 2 == start_part))
        def _():
            each(1, NZ, lambda k: field_copy(u, j, k).start())
            slab = me if u == 0 else partner
            gbuf[u, j, pl.ds(spot, 1)] = fbuf[j, pl.ds(slab, 1)]

    def backward(j, carry):
        for n in range(2):
            ns = pl.ds(n * NY, NY)
            rh, rl = rhi[j, :, ns], rlo[j, :, ns]
            u = mm(whi[...], rh) + mm(wlo[...], rh) + mm(whi[...], rl)
            uhi[:, ns], ulo[:, ns] = split(u)
        uh, ul = uhi[...], ulo[...]
        f = mm(uh, thi[...]) + mm(uh, tlo[...]) + mm(ul, thi[...])
        fbuf[j] = f.reshape(SPACE, NROW, NY)
        send_fields(1, j)

        @pl.when(special & (j % 2 != start_part))
        def _():
            each(1, SPACE, lambda k: return_copy(j // 2, k).start())
            hbuf[1 - hi, pl.ds(j // 2, 1)] = fbuf[j, pl.ds(me, 1)]

        return carry

    lax.fori_loop(0, 1, backward, 0)
    line = line_of([local_energy[0] + first_share, local_energy[1] + second_share])
    msg_e[...] = line
    got_e[1, me] = line
    lax.fori_loop(1, SPACE, lambda k, x: (energy_copy(SPACE - k).start(), x)[1], 0)
    at_images(
        lambda other, slot: each(
            0, SPACE, lambda k: image_energy_copy(other, slot, k).start()
        )
    )

    lax.fori_loop(1, 6, backward, 0)
    each(0, 6, lambda j: send_fields(0, j))

    def wait_fields(u, j):
        full = special | (j % 2 == start_part)

        @pl.when(full)
        def _():
            wait_bytes(gbuf.at[u, j, pl.ds(0, NZ - 1)], f_r.at[u, j])

        @pl.when(jnp.logical_not(full))
        def _():
            wait_bytes(gbuf.at[u, j, pl.ds(0, NZ - 2)], f_r.at[u, j])

    def layers_back(u, c, put):
        for part in range(2):
            wait_fields(u, 2 * c + part)
        half = NZ // 2
        for h in range(2):
            @pl.when(hi == h)
            def _(h=h):
                sums = {False: [None] * half, True: [None] * half}
                for t, part, sine, q in plane_sides(h):
                    v = gbuf[u, 2 * c + part, t]
                    acc = sums[sine]
                    for n in range(half):
                        term = v * layer_wave(q, n, sine)
                        acc[n] = term if acc[n] is None else acc[n] + term
                even, odd = sums[False], sums[True]
                for n in range(half):
                    put(h, n, even[n] + odd[n])
                    put(h, NZ - 1 - n, even[n] - odd[n])

    def result_copy(c):
        return remote(obuf.at[c], rbuf.at[c], o_s.at[c], o_r.at[c], partner)

    def partner_result(c):
        def put(h, n, value):
            obuf[c, n] = value

        layers_back(1, c, put)
        result_copy(c).start()

    each(0, 3, partner_result)

    @pl.when(has_prior)
    def _():
        image_copy(im_next, 0).wait_recv()

    @pl.when(has_next)
    def _():
        image_copy(im_prior, 1).wait_recv()

    @pl.when(jnp.logical_not(has_prior))
    def _():
        prior[...] = m[0]

    @pl.when(jnp.logical_not(has_next))
    def _():
        nxt[...] = m[1]


    def angle_squared(a, b):
        n0 = a[1] * b[2] - a[2] * b[1]
        n1 = a[2] * b[0] - a[0] * b[2]
        n2 = a[0] * b[1] - a[1] * b[0]
        sine = jnp.sqrt(n0 * n0 + n1 * n1 + n2 * n2)
        cosine = a[0] * b[0] + a[1] * b[1] + a[2] * b[2]
        angle = jnp.arctan2(sine, cosine)
        return angle * angle

    def distances(z, acc):
        p = [prior[c, z] for c in range(3)]
        a = [m[0, c, z] for c in range(3)]
        b = [m[1, c, z] for c in range(3)]
        n = [nxt[c, z] for c in range(3)]
        return (
            acc[0] + angle_squared(a, p),
            acc[1] + angle_squared(a, b),
            acc[2] + angle_squared(b, n),
        )

    flat = jnp.zeros((NROW, NY), F32)
    spans = [total(x) for x in lax.fori_loop(0, NZ, distances, (flat, flat, flat))]

    mine = got_e.at[1, pl.ds(0, SPACE - 1)]
    wait_bytes(mine, e_r)
    for present, group, slot in ((has_prior, 0, 0), (has_next, 2, 1)):
        @pl.when(present)
        def _(group=group, slot=slot):
            wait_bytes(got_e.at[group], n_r.at[slot])

        @pl.when(jnp.logical_not(present))
        def _(group=group):
            got_e[group] = got_e[1]

    e_prior, e_own, e_next = (-0.5 * sum_round(got_e.at[g]) for g in range(3))
    tile_x[0] = e_own / CELLS

    line = [e_prior[0:1, 1:2], e_own[0:1, 0:1], e_own[0:1, 1:2], e_next[0:1, 0:1]]
    lengths = []
    for i in range(2):
        rise_next = line[i + 2] - line[i + 1]
        rise_prior = line[i + 1] - line[i]
        upward = (rise_next > 0) & (rise_prior > 0)
        downward = (rise_next < 0) & (rise_prior < 0)
        larger = jnp.maximum(jnp.abs(rise_next), jnp.abs(rise_prior))
        smaller = jnp.minimum(jnp.abs(rise_next), jnp.abs(rise_prior))
        toward_next = line[i + 2] > line[i]
        one, nil = jnp.ones((1, 1), F32), jnp.zeros((1, 1), F32)
        w_next = jnp.where(
            upward, one, jnp.where(downward, nil, jnp.where(toward_next, larger, smaller))
        )
        w_prior = jnp.where(
            upward, nil, jnp.where(downward, one, jnp.where(toward_next, smaller, larger))
        )
        w_next = jnp.broadcast_to(w_next, (NROW, NY))
        w_prior = jnp.broadcast_to(w_prior, (NROW, NY))

        def tangent(z, acc, i=i, w_next=w_next, w_prior=w_prior):
            own = [m[i, c, z] for c in range(3)]
            ahead = [m[1, c, z] if i == 0 else nxt[c, z] for c in range(3)]
            behind = [prior[c, z] if i == 0 else m[0, c, z] for c in range(3)]
            v = [
                w_next * (ahead[c] - own[c]) + w_prior * (own[c] - behind[c]) for c in range(3)
            ]
            along = v[0] * own[0] + v[1] * own[1] + v[2] * own[2]
            for c in range(3):
                t = v[c] - along * own[c]
                tang[i, c, z] = t
                acc = acc + t * t
            return acc

        lengths.append(total(lax.fori_loop(0, NZ, tangent, flat)))

    for t in range(2):
        @pl.when(me != (1 - t) * NZ)
        def _(t=t):
            wait_bytes(hbuf.at[t], g_r.at[t])

    def own_result(c):
        def put(h, n, value):
            floc[h, c, n] = floc[h, c, n] + value

        layers_back(0, c, put)
        result_copy(c).wait_recv()
        for n in range(NZ):
            floc[1 - hi, c, n] = floc[1 - hi, c, n] + rbuf[c, n]
            floc[0, c, n] = floc[0, c, n] + hbuf[0, c] * layer_wave(NZ, n, True)
            floc[1, c, n] = floc[1, c, n] + hbuf[1, c] * layer_wave(0, n, False)

    each(0, 3, own_result)

    drives = []
    for i in range(2):
        def force(z, acc, i=i):
            own = [m[i, c, z] for c in range(3)]
            f = [floc[i, c, z] for c in range(3)]
            along = f[0] * own[0] + f[1] * own[1] + f[2] * own[2]
            for c in range(3):
                t = f[c] - along * own[c]
                floc[i, c, z] = t
                acc = acc + t * tang[i, c, z]
            return acc

        drives.append(total(lax.fori_loop(0, NZ, force, flat)))

    send_round(round_c, msg_c, got_c, line_of(lengths + drives + spans))
    round_c[1]()
    sums = sum_round(got_c)
    dist = [jnp.sqrt(sums[0:1, 4 + j : 5 + j] / CELLS) for j in range(3)]
    tops = []
    for i in range(2):
        scale = jnp.sqrt(sums[0:1, i : i + 1] / CELLS + epsilon)
        parallel = sums[0:1, 2 + i : 3 + i] / (CELLS * scale)
        spring = spring_strength * (dist[i + 1] - dist[i])
        index = 2 * im + i
        interior = (index > 0) & (index < 2 * images - 1)
        coef = jnp.broadcast_to((spring - parallel) / scale, (NROW, NY))
        inner = jnp.where(interior, 1, 0)

        def band(z, acc, i=i, coef=coef, inner=inner):
            size = None
            for c in range(3):
                b = floc[i, c, z] + coef * tang[i, c, z]
                b = jnp.where(inner > 0, b, 0.0)
                out_b[i, c, z] = b
                size = b * b if size is None else size + b * b
            return jnp.maximum(acc, size)

        top = lax.fori_loop(0, NZ, band, flat)
        tops.append(jnp.max(jnp.max(top, axis=0, keepdims=True), axis=1, keepdims=True))

    send_round(round_d, msg_d, got_d, line_of(tops))
    round_d[1]()
    largest = got_d[0]
    for s in range(1, SPACE):
        largest = jnp.maximum(largest, got_d[s])
    largest = jnp.sqrt(largest)
    tile_x[1] = largest

    def drain(k):
        @pl.when(near(k) % NZ != 0)
        def _():
            wait_bytes(sbuf.at[0, pl.ds(0, 2)], y_s.at[k])

        @pl.when(near(k) % NZ == 0)
        def _():
            wait_bytes(sbuf.at[0, 0], y_s.at[k])

        @pl.when(special)
        def _():
            wait_bytes(sbuf.at[0, 0], f_s.at[k])

        @pl.when(jnp.logical_not(special))
        def _():
            wait_bytes(sbuf.at[0, pl.ds(0, 2)], f_s.at[k])

    each(1, NZ, drain)

    @pl.when(special)
    def _():
        wait_bytes(fbuf.at[pl.ds(0, 3), pl.ds(0, SPACE - 1)], g_s)

    for t in range(2):
        @pl.when(me != t * NZ)
        def _(t=t):
            wait_bytes(xbuf.at[t], x_s.at[t])

    each(0, 3, lambda c: partner_copy(c).wait_send())
    each(0, 3, lambda c: result_copy(c).wait_send())
    for rnd in (round_c, round_d):
        rnd[2]()
    wait_bytes(mine, e_s)
    at_images(lambda other, slot: wait_bytes(got_e.at[2 * slot], n_s.at[slot]))
    at_images(lambda other, slot: image_copy(other, slot).wait_send())
    at_slabs(lambda side: halo_copy(side).wait_send())


def finish_kernel(m_ref, b_ref, tile_ref, upd_hbm, bf_hbm, en_ref, upd, sem):
    stores = [pltpu.make_async_copy(b_ref, bf_hbm, sem.at[2])]
    stores[0].start()
    for i in range(2):
        en_ref[i] = jnp.max(tile_ref[0, :, i : i + 1])
        move = jnp.minimum(
            step_limit, rotation_limit / (tile_ref[1, :, i : i + 1] + epsilon)
        )
        move = jnp.broadcast_to(move, (NROW, NY))

        def advance(z, carry, i=i, move=move):
            s = [m_ref[i, c, z] + move * b_ref[i, c, z] for c in range(3)]
            length = jnp.sqrt(s[0] * s[0] + s[1] * s[1] + s[2] * s[2])
            for c in range(3):
                upd[i, c, z] = s[c] / length
            return carry

        lax.fori_loop(0, NZ, advance, 0)
        stores.append(pltpu.make_async_copy(upd.at[i], upd_hbm.at[i], sem.at[i]))
        stores[-1].start()
    for c in stores:
        c.wait()


def body(magnet, anisotropy, kernel):
    table = wave_table(NX)
    across = np.concatenate(split_table(np.ascontiguousarray(table.T)), axis=1)
    tables = jnp.asarray(np.concatenate([*split_table(table), across], axis=0))
    slab = (2, 3, NZ, NROW, NY)
    vm = pltpu.VMEM
    dma = pltpu.SemaphoreType.DMA
    tile = (1, 128)
    scratch = [
        vm(slab[1:], F32), vm(slab[1:], F32),
        vm((2, 2, 3, NZ, NY), F32), vm((2, 2, 3, NZ, NY), F32),
        vm(slab[1:], F32), vm((2, 3, NROW, NY), F32),
        vm((2, NZ, 6, NROW, NY), F32), vm((6, SPACE, NROW, NY), F32),
        vm((NX, 2 * NY), BF16), vm((NX, 2 * NY), BF16),
        vm((6, 2 * NX, 2 * NY), F32),
        vm((6, 2 * NX, 2 * NY), BF16), vm((6, 2 * NX, 2 * NY), BF16),
        vm((6, NX + 8, NY + 128), F32), vm((6, 2 * NX, 2 * NY), F32),
        vm((NX, 2 * NY), BF16), vm((NX, 2 * NY), BF16),
        vm((6, SPACE, NROW, NY), F32), vm((2, 6, NZ, NROW, NY), F32),
        vm(slab[1:], F32), vm(slab[1:], F32), vm((2, 3, NROW, NY), F32),
        vm(slab, F32), vm(slab, F32),
        vm((2 * NX, 2 * NY), BF16), vm((2, 2 * NX, NY), BF16), pltpu.SMEM((NROW,), F32),
        vm(tile, F32), vm((3, SPACE, *tile), F32),
        vm(tile, F32), vm((SPACE, *tile), F32),
        vm(tile, F32), vm((SPACE, *tile), F32),
        dma((6,)),
        dma((3,)), dma((3,)), dma((2,)), dma((3,)),
        dma((NZ,)), dma((6,)), dma((NZ,)), dma((2, 6)), dma, dma((2,)), dma((3,)), dma((3,)),
        dma, dma, dma((2,)), dma((2,)), dma, dma, dma, dma,
        dma((2,)), dma((2,)), dma((2,)), dma((2,)),
    ]
    hbm = pl.BlockSpec(memory_space=pltpu.HBM)
    vmem = pl.BlockSpec(memory_space=pltpu.VMEM)
    smem = pl.BlockSpec(memory_space=pltpu.SMEM)
    own, band, tiles = pl.pallas_call(
        step_kernel,
        out_shape=(
            jax.ShapeDtypeStruct(slab, F32),
            jax.ShapeDtypeStruct(slab, F32),
            jax.ShapeDtypeStruct((2, *tile), F32),
        ),
        in_specs=[hbm] * 4,
        out_specs=(vmem, vmem, vmem),
        scratch_shapes=scratch,
        compiler_params=pltpu.CompilerParams(
            collective_id=0, has_side_effects=True, vmem_limit_bytes=STEP_VMEM
        ),
        name="band_step",
    )(magnet, anisotropy, kernel, tables)
    return pl.pallas_call(
        finish_kernel,
        out_shape=(
            jax.ShapeDtypeStruct(slab, F32),
            jax.ShapeDtypeStruct(slab, F32),
            jax.ShapeDtypeStruct((2,), F32),
        ),
        in_specs=[vmem, vmem, vmem],
        out_specs=(hbm, hbm, smem),
        scratch_shapes=[vm(slab, F32), dma((3,))],
        compiler_params=pltpu.CompilerParams(vmem_limit_bytes=3 * 2**20),
        name="band_finish",
    )(own, band, tiles)


def solution(mesh):
    in_specs = (P("image", None, None, "space", None), P("space"), P(None, "space", None, None))
    out_specs = (
        P("image", None, None, "space", None),
        P("image", None, None, "space", None),
        P("image"),
    )
    return jax.shard_map(body, mesh=mesh, in_specs=in_specs, out_specs=out_specs, check_vma=False)
```

```python
import math

import jax
import jax.numpy as jnp
import numpy as np
from jax import lax
from jax.experimental import pallas as pl
from jax.experimental.pallas import tpu as pltpu
from jax.sharding import PartitionSpec as P

F32 = jnp.float32
BF16 = jnp.bfloat16
MESH = pl.DeviceIdType.MESH

exchange_strength = 0.25
chiral_strength = 0.3
spring_strength = 10.0
step_limit = 1.0
rotation_limit = 0.5
epsilon = 1e-06

NZ, NROW, NY, NX = 8, 16, 256, 256
SPACE = 16
CELLS = NZ * NX * NY
STEP_VMEM = 53200 * 1024


def split_table(table):
    high = table.astype(np.dtype(BF16))
    low = (table - high.astype(np.float64)).astype(np.dtype(BF16))
    return high, low


def wave_table(count):
    position = 2 * np.arange(count)[:, None] - (count - 1)
    cosine = np.arange(count)[None, :]
    sine = np.where(cosine == 0, count, cosine)
    unit = 2.0 * math.pi / (4 * count)
    return np.concatenate(
        [
            np.cos((cosine * position % (4 * count)) * unit),
            np.sin((sine * position % (4 * count)) * unit),
        ],
        axis=1,
    )


def layer_wave(q, n, sine):
    angle = 2.0 * math.pi * q * (n - (NZ - 1) / 2) / (2 * NZ)
    return float(math.sin(angle) if sine else math.cos(angle))


def split(x):
    high = x.astype(BF16)
    low = (x - high.astype(F32)).astype(BF16)
    return high, low


def mm(a, b):
    return jnp.dot(a, b, preferred_element_type=F32)


def total(x):
    return jnp.sum(jnp.sum(x, axis=0, keepdims=True), axis=1, keepdims=True)


def line_of(values):
    lane = lax.broadcasted_iota(jnp.int32, (1, 128), 1)
    line = jnp.zeros((1, 128), F32)
    for j, v in enumerate(values):
        line = jnp.where(lane == j, v, line)
    return line


def step_kernel(
    m_hbm, ani_hbm, k_hbm, tab_hbm,
    m, out_b, tile_x,
    prior, nxt, halo_out, halo_in, pbuf, xbuf, sbuf, ybuf, zhi, zlo, spec, rhi, rlo,
    kraw, keff, uhi, ulo, fbuf, gbuf, obuf, rbuf, hbuf, floc, tang,
    wtab, ttab, ani_ref,
    msg_e, got_e, msg_c, got_c, msg_d, got_d,
    in_sem, p_s, p_r, x_s, x_r, y_s, y_r, f_s, f_r, g_s, g_r, o_s, o_r,
    e_s, e_r, n_s, n_r, c_s, c_r, d_s, d_r, i_s, i_r, h_s, h_r,
):
    im = lax.axis_index("image")
    me = lax.axis_index("space")
    images = lax.axis_size("image")
    hi, spot = me // NZ, me % NZ
    partner = (1 - hi) * NZ + spot
    special = spot == 0

    def dest(k):
        return (me + k) % SPACE

    def piece(c, part):
        if isinstance(c, int):
            return 3 * (1 - part if c == 2 else part) + c
        return 3 * jnp.where(c == 2, 1 - part, part) + c

    def part_of(j):
        return jnp.where(j % 3 == 2, 1 - j // 3, j // 3)

    def is_regular(j):
        return jnp.logical_not(special) | (part_of(j) == hi)

    def near(k):
        return hi * NZ + (spot + k) % NZ

    def each(lo, up, do):
        lax.fori_loop(lo, up, lambda k, x: (do(k), x)[1], 0)

    def remote(src, dst, send, recv, device):
        return pltpu.make_async_remote_copy(
            src_ref=src, dst_ref=dst, send_sem=send, recv_sem=recv,
            device_id={"space": device}, device_id_type=MESH,
        )

    def wait_bytes(ref, sem):
        pltpu.make_async_copy(ref, ref, sem).wait()

    def plane_sides(h):
        rows = [(0, h, h == 1, NZ * h)]
        for t in range(1, NZ):
            rows += [(t, 0, False, NZ * h + t), (t, 1, True, NZ * h + t)]
        return rows

    def layer_sums(lines):
        half = NZ // 2
        even = [lines[n] + lines[NZ - 1 - n] for n in range(half)]
        odd = [lines[n] - lines[NZ - 1 - n] for n in range(half)]
        return even, odd

    def layer_dot(terms, q, sine):
        acc = terms[0] * layer_wave(q, 0, sine)
        for n in range(1, NZ // 2):
            acc = acc + terms[n] * layer_wave(q, n, sine)
        return acc

    has_next, has_prior = im < images - 1, im > 0
    im_next = jnp.minimum(im + 1, images - 1)
    im_prior = jnp.maximum(im - 1, 0)
    sp_next = jnp.minimum(me + 1, SPACE - 1)
    sp_prior = jnp.maximum(me - 1, 0)

    loads = [
        pltpu.make_async_copy(tab_hbm.at[pl.ds(0, 2 * NX)], wtab, in_sem.at[0]),
        pltpu.make_async_copy(
            tab_hbm.at[pl.ds(2 * NX, 2 * NX), pl.ds(0, NY)], ttab.at[0], in_sem.at[1]
        ),
        pltpu.make_async_copy(
            tab_hbm.at[pl.ds(2 * NX, 2 * NX), pl.ds(NY, NY)], ttab.at[1], in_sem.at[2]
        ),
        pltpu.make_async_copy(ani_hbm, ani_ref, in_sem.at[3]),
        pltpu.make_async_copy(
            k_hbm.at[:, 0, pl.ds(0, NX + 8), pl.ds(0, NY + 128)], kraw, in_sem.at[4]
        ),
    ]
    load_m = pltpu.make_async_copy(m_hbm, m, in_sem.at[5])
    load_m.start()
    for c in loads:
        c.start()
    whi, wlo = wtab.at[pl.ds(0, NX)], wtab.at[pl.ds(NX, NX)]
    thi, tlo = ttab.at[0], ttab.at[1]

    barrier = pltpu.get_barrier_semaphore()

    def greet(k, carry):
        pl.semaphore_signal(barrier, inc=1, device_id={"space": dest(k)}, device_id_type=MESH)
        return carry

    lax.fori_loop(1, SPACE, greet, 0)

    def at_images(do):
        for present, other, slot in ((has_next, im_next, 0), (has_prior, im_prior, 1)):
            @pl.when(present)
            def _(other=other, slot=slot):
                do(other, slot)

    at_images(
        lambda other, slot: each(
            0, SPACE,
            lambda k: pl.semaphore_signal(
                barrier, inc=1, device_id={"image": other, "space": k}, device_id_type=MESH
            ),
        )
    )
    greeted = SPACE - 1 + SPACE * (jnp.minimum(im, 1) + jnp.minimum(images - 1 - im, 1))

    load_m.wait()
    def layers_in(u, c, line):
        for h in range(2):
            @pl.when(hi == h)
            def _(h=h):
                even, odd = layer_sums([line(h, n) for n in range(NZ)])
                for t, part, sine, q in plane_sides(h):
                    sbuf[u, t, piece(c, part)] = layer_dot(odd if sine else even, q, sine)

    def own_layers(c):
        layers_in(0, c, lambda h, n: m[h, c, n])
        even, _ = layer_sums([m[1, c, n] for n in range(NZ)])
        _, odd = layer_sums([m[0, c, n] for n in range(NZ)])
        xbuf[0, c] = layer_dot(even, 0, False)
        xbuf[1, c] = layer_dot(odd, NZ, True)

    each(0, 3, own_layers)

    for i in range(2):
        for c in range(3):
            halo_out[0, i, c] = m[i, c, :, 0, :]
            halo_out[1, i, c] = m[i, c, :, NROW - 1, :]

    pl.semaphore_wait(barrier, greeted)

    def partner_copy(c):
        return remote(m.at[1 - hi, c], pbuf.at[c], p_s.at[c], p_r.at[c], partner)

    def plane_copy(u, j, k):
        to = near(k)
        slab = me if u == 0 else partner
        return remote(
            sbuf.at[u, to % NZ, j], ybuf.at[j, slab], y_s.at[k], y_r.at[j], to
        )

    def extra_copy(t, c):
        return remote(
            xbuf.at[t, c], ybuf.at[piece(c, 1 - t), me], x_s.at[t], x_r.at[c], t * NZ
        )

    def send_planes(u, first, last):
        def one(j):
            def to(k):
                @pl.when((near(k) % NZ != 0) | (part_of(j) == hi))
                def _():
                    plane_copy(u, j, k).start()

            each(1, NZ, to)

            @pl.when(is_regular(j))
            def _():
                slab = me if u == 0 else partner
                ybuf[j, pl.ds(slab, 1)] = sbuf[u, spot, pl.ds(j, 1)]

        each(first, last, one)

    def halo_copy(side):
        return remote(
            halo_out.at[side], halo_in.at[1 - side], h_s.at[side], h_r.at[side],
            (sp_prior, sp_next)[side],
        )

    def at_slabs(do):
        for side, present in ((0, me > 0), (1, me < SPACE - 1)):
            @pl.when(present)
            def _(side=side):
                do(side)

    def image_copy(other, slot):
        return pltpu.make_async_remote_copy(
            src_ref=m.at[1 - slot], dst_ref=(prior, nxt)[slot], send_sem=i_s.at[slot],
            recv_sem=i_r.at[slot], device_id={"image": other}, device_id_type=MESH,
        )

    at_slabs(lambda side: halo_copy(side).start())
    for t in range(2):
        @pl.when(me != t * NZ)
        def _(t=t):
            each(0, 3, lambda c: extra_copy(t, c).start())

        @pl.when(me == t * NZ)
        def _(t=t):
            for c in range(3):
                ybuf[piece(c, 1 - t), pl.ds(me, 1)] = xbuf[t, pl.ds(c, 1)]

    each(0, 3, lambda c: partner_copy(c).start())
    send_planes(0, 0, 6)

    loads[4].wait()
    plane_weight = jnp.where(me % NZ == 0, 1.0, 2.0) * (-4.0 / (2 * NZ * 2 * NX * 2 * NY))
    lane = lax.broadcasted_iota(jnp.int32, (64, 128), 1)

    def prepare(t, carry):
        comp, first = t // 4, pl.multiple_of((t % 4) * 64, 64)
        row = lax.broadcasted_iota(jnp.int32, (64, NY), 0) + first
        column = lax.broadcasted_iota(jnp.int32, (64, NY), 1)
        weight = plane_weight * jnp.where(row == 0, 0.5, 1.0) * jnp.where(column == 0, 0.5, 1.0)
        base = kraw[comp, pl.ds(first, 64), pl.ds(0, NY)]
        edge = kraw[comp, pl.ds(first, 64), pl.ds(NY, 128)]
        last = kraw[comp, pl.ds(NX, 8), pl.ds(0, NY)][0:1]
        last_edge = kraw[comp, pl.ds(NX, 8), pl.ds(NY, 128)][0:1]
        top = row == 0
        for bx in range(2):
            body_part = jnp.where(top, last, base) if bx else base
            edge_part = jnp.where(top[:, :128], last_edge, edge) if bx else edge
            for by in range(2):
                if by:
                    left = jnp.where(lane == 0, edge_part, body_part[:, :128])
                    value = jnp.concatenate([left, body_part[:, 128:]], axis=1)
                else:
                    value = body_part
                keff[comp, pl.ds(bx * NX + first, 64), pl.ds(by * NY, NY)] = value * weight
        return carry

    lax.fori_loop(0, 24, prepare, 0)

    def partner_layers(c):
        partner_copy(c).wait_recv()
        layers_in(1, c, lambda h, n: pbuf[c, n])
        send_planes(1, c, c + 1)

    partner_layers(0)

    @pl.when(me < SPACE - 1)
    def _():
        halo_copy(0).wait_recv()

    @pl.when(me > 0)
    def _():
        halo_copy(1).wait_recv()

    row = lax.broadcasted_iota(jnp.int32, (NROW, NY), 0)
    column = lax.broadcasted_iota(jnp.int32, (NROW, NY), 1)
    loads[3].wait()
    easy = jnp.zeros((NROW, NY), F32)
    for r in range(NROW):
        easy = jnp.where(row == r, 2.0 * ani_ref[r], easy)
    edges = (
        jnp.where((row == 0) & (me == 0), 1.0, 0.0)
        + jnp.where((row == NROW - 1) & (me == SPACE - 1), 1.0, 0.0)
        + jnp.where(column == 0, 1.0, 0.0)
        + jnp.where(column == NY - 1, 1.0, 0.0)
    )

    def local_part(i):
        def layer(z, acc):
            at_bottom = z == 0
            at_top = z == NZ - 1
            present = 6.0 - edges - jnp.where(at_bottom | at_top, 1.0, 0.0)
            own, xp, xm, yp, ym, field = [], [], [], [], [], []
            for c in range(3):
                v = m[i, c, z]
                before = jnp.where(me == 0, 0.0, halo_in[0, i, c, pl.ds(z, 1), :])
                after = jnp.where(me == SPACE - 1, 0.0, halo_in[1, i, c, pl.ds(z, 1), :])
                own.append(v)
                xp.append(jnp.where(row == NROW - 1, after, pltpu.roll(v, NROW - 1, 0)))
                xm.append(jnp.where(row == 0, before, pltpu.roll(v, 1, 0)))
                yp.append(jnp.where(column == NY - 1, 0.0, pltpu.roll(v, NY - 1, 1)))
                ym.append(jnp.where(column == 0, 0.0, pltpu.roll(v, 1, 1)))
                zp = jnp.where(at_top, 0.0, m[i, c, jnp.minimum(z + 1, NZ - 1)])
                zm = jnp.where(at_bottom, 0.0, m[i, c, jnp.maximum(z - 1, 0)])
                around = xp[c] + xm[c] + yp[c] + ym[c] + zp + zm
                field.append(exchange_strength * (around - present * v))
            field[0] = field[0] + chiral_strength * (xp[2] - xm[2])
            field[1] = field[1] + chiral_strength * (yp[2] - ym[2])
            field[2] = (
                field[2]
                - chiral_strength * ((xp[0] - xm[0]) + (yp[1] - ym[1]))
                + easy * own[2]
            )
            for c in range(3):
                floc[i, c, z] = field[c]
                acc = acc + field[c] * own[c]
            return acc

        return lax.fori_loop(0, NZ, layer, jnp.zeros((NROW, NY), F32))

    local_energy = [total(local_part(0))]
    partner_layers(1)
    local_energy.append(total(local_part(1)))
    partner_layers(2)
    send_planes(1, 3, 6)
    at_images(lambda other, slot: image_copy(other, slot).start())

    for c in loads[0:3]:
        c.wait()

    def forward(j, carry):
        regular = is_regular(j)

        @pl.when(regular)
        def _():
            wait_bytes(ybuf.at[j, pl.ds(0, SPACE - 2)], y_r.at[j])

        @pl.when(jnp.logical_not(regular))
        def _():
            wait_bytes(ybuf.at[j, pl.ds(0, SPACE - 1)], x_r.at[j % 3])

        high, low = split(ybuf[j].reshape(NX, NY))
        for n in range(2):
            ns = pl.ds(n * NY, NY)
            out = mm(high, whi[:, ns]) + mm(high, wlo[:, ns]) + mm(low, whi[:, ns])
            zhi[:, ns], zlo[:, ns] = split(out)
        for r in range(2):
            for n in range(2):
                rs, ns = pl.ds(r * NX, NX), pl.ds(n * NY, NY)
                zh, zl = zhi[:, ns], zlo[:, ns]
                spec[j, rs, ns] = mm(thi[rs, :], zh) + mm(tlo[rs, :], zh) + mm(thi[rs, :], zl)
        return carry

    def respond(g):
        def block(t, acc):
            for half in range(2):
                acc = quarter(pl.multiple_of(t * 16, 16), half * 128, acc)
            return acc

        def quarter(r0, l0, acc):
            def at(bx, by):
                return (pl.ds(bx * NX + r0, 16), pl.ds(by * NY + l0, 128))

            parts = (g, g, 1 - g)
            v = {
                (c, bx, by): spec[(3 * g + c, *at(bx, by))]
                for c in range(3) for bx in range(2) for by in range(2)
            }
            sums = list(acc)

            def plus(x, minus, y):
                return x - y if minus else x + y

            for bx in range(2):
                for by in range(2):
                    here = at(bx, by)
                    k = [keff[(comp, *here)] for comp in range(6)]
                    fx = plus(k[0] * v[0, bx, by], bx == by, k[3] * v[1, 1 - bx, 1 - by])
                    fx = plus(fx, parts[0] == bx, k[4] * v[2, 1 - bx, by])
                    fy = plus(k[1] * v[1, bx, by], bx == by, k[3] * v[0, 1 - bx, 1 - by])
                    fy = plus(fy, parts[1] == by, k[5] * v[2, bx, 1 - by])
                    fz = plus(k[2] * v[2, bx, by], parts[2] == bx, k[4] * v[0, 1 - bx, by])
                    fz = plus(fz, parts[2] == by, k[5] * v[1, bx, 1 - by])
                    sums[0] = sums[0] + (fx * v[0, bx, by] + fy * v[1, bx, by])
                    sums[1] = sums[1] + fz * v[2, bx, by]
                    for c, f in enumerate((fx, fy, fz)):
                        rhi[(3 * g + c, *here)], rlo[(3 * g + c, *here)] = split(f)
            return tuple(sums)

        zero = jnp.zeros((16, 128), F32)
        flat_sum, z_sum = lax.fori_loop(0, 16, block, (zero, zero))
        return (flat_sum, z_sum) if g == 0 else (z_sum, flat_sum)

    def small_round(msg, got, s_sem, r_sem):
        def copy(k):
            return pltpu.make_async_remote_copy(
                src_ref=msg, dst_ref=got.at[me], send_sem=s_sem,
                recv_sem=r_sem, device_id={"space": dest(k)}, device_id_type=MESH,
            )

        part = got.at[pl.ds(0, SPACE - 1)]

        def start():
            lax.fori_loop(1, SPACE, lambda k, x: (copy(k).start(), x)[1], 0)

        def finish():
            pltpu.make_async_copy(part, part, r_sem).wait()

        def drain():
            pltpu.make_async_copy(part, part, s_sem).wait()

        return start, finish, drain

    def send_round(rnd, msg, got, tile):
        msg[...] = tile
        got[me] = tile
        rnd[0]()

    def sum_round(got):
        acc = got[0]
        for s in range(1, SPACE):
            acc = acc + got[s]
        return acc

    round_c = small_round(msg_c, got_c, c_s, c_r)
    round_d = small_round(msg_d, got_d, d_s, d_r)

    def energy_copy(k):
        return pltpu.make_async_remote_copy(
            src_ref=msg_e, dst_ref=got_e.at[1, me], send_sem=e_s,
            recv_sem=e_r, device_id={"space": dest(k)}, device_id_type=MESH,
        )

    def image_energy_copy(other, slot, k):
        return pltpu.make_async_remote_copy(
            src_ref=msg_e, dst_ref=got_e.at[2 * slot, me], send_sem=n_s.at[slot],
            recv_sem=n_r.at[slot], device_id={"image": other, "space": k},
            device_id_type=MESH,
        )

    def field_copy(u, j, k):
        to = near(k)
        slab = to if u == 0 else (1 - hi) * NZ + to % NZ
        return remote(
            fbuf.at[j, slab], gbuf.at[u, j, spot], f_s.at[k], f_r.at[u, j], to
        )

    def return_copy(c, k):
        part = 1 - hi
        to = dest(k)
        return remote(
            fbuf.at[piece(c, part), to], hbuf.at[1 - hi, c], g_s, g_r.at[1 - hi], to
        )

    def send_fields(u, j):
        @pl.when(is_regular(j))
        def _():
            each(1, NZ, lambda k: field_copy(u, j, k).start())
            slab = me if u == 0 else partner
            gbuf[u, j, pl.ds(spot, 1)] = fbuf[j, pl.ds(slab, 1)]

    def backward(j, carry):
        for n in range(2):
            ns = pl.ds(n * NY, NY)
            rh, rl = rhi[j, :, ns], rlo[j, :, ns]
            u = mm(whi[...], rh) + mm(wlo[...], rh) + mm(whi[...], rl)
            uhi[:, ns], ulo[:, ns] = split(u)
        uh, ul = uhi[...], ulo[...]
        f = mm(uh, thi[...]) + mm(uh, tlo[...]) + mm(ul, thi[...])
        fbuf[j] = f.reshape(SPACE, NROW, NY)
        send_fields(1, j)

        @pl.when(jnp.logical_not(is_regular(j)))
        def _():
            each(1, SPACE, lambda k: return_copy(j % 3, k).start())
            hbuf[1 - hi, pl.ds(j % 3, 1)] = fbuf[j, pl.ds(me, 1)]

        return carry

    def wait_fields(u, j):
        full = special | (part_of(j) == hi)

        @pl.when(full)
        def _():
            wait_bytes(gbuf.at[u, j, pl.ds(0, NZ - 1)], f_r.at[u, j])

        @pl.when(jnp.logical_not(full))
        def _():
            wait_bytes(gbuf.at[u, j, pl.ds(0, NZ - 2)], f_r.at[u, j])

    def half_layers(u, j, put):
        wait_fields(u, j)
        for h in range(2):
            for part in range(2):
                @pl.when((hi == h) & (part_of(j) == part))
                def _(h=h, part=part):
                    sums = [None] * (NZ // 2)
                    for t, own_part, sine, q in plane_sides(h):
                        if own_part != part:
                            continue
                        v = gbuf[u, j, t]
                        for n in range(NZ // 2):
                            term = v * layer_wave(q, n, sine)
                            sums[n] = term if sums[n] is None else sums[n] + term
                    for n in range(NZ // 2):
                        put(n, sums[n])

    def result_copy(j):
        return remote(obuf.at[j], rbuf.at[j], o_s.at[j], o_r.at[j], partner)

    def partner_result(j):
        def put(n, value):
            obuf[j, n] = value

        half_layers(1, j, put)
        result_copy(j).start()

    lax.fori_loop(0, 3, forward, 0)
    first_a, first_b = respond(0)
    lax.fori_loop(0, 3, backward, 0)
    each(0, 3, lambda j: send_fields(0, j))
    lax.fori_loop(3, 6, forward, 0)
    second_a, second_b = respond(1)
    part_a, part_b = total(first_a + second_a), total(first_b + second_b)
    none = jnp.zeros((1, 1), F32)
    first_share = jnp.where(me <= NZ, part_a, none) + jnp.where(
        (me >= 1) & (me < NZ), part_b, none
    )
    second_share = jnp.where(me > NZ, part_a, none) + jnp.where(
        (me == 0) | (me >= NZ), part_b, none
    )
    line = line_of([local_energy[0] + first_share, local_energy[1] + second_share])
    msg_e[...] = line
    got_e[1, me] = line
    lax.fori_loop(1, SPACE, lambda k, x: (energy_copy(SPACE - k).start(), x)[1], 0)
    at_images(
        lambda other, slot: each(
            0, SPACE, lambda k: image_energy_copy(other, slot, k).start()
        )
    )

    each(0, 3, partner_result)
    lax.fori_loop(3, 4, backward, 0)
    lax.fori_loop(4, 6, backward, 0)
    each(3, 6, lambda j: send_fields(0, j))

    each(3, 6, partner_result)

    @pl.when(has_prior)
    def _():
        image_copy(im_next, 0).wait_recv()

    @pl.when(has_next)
    def _():
        image_copy(im_prior, 1).wait_recv()

    @pl.when(jnp.logical_not(has_prior))
    def _():
        prior[...] = m[0]

    @pl.when(jnp.logical_not(has_next))
    def _():
        nxt[...] = m[1]


    def angle_squared(a, b):
        n0 = a[1] * b[2] - a[2] * b[1]
        n1 = a[2] * b[0] - a[0] * b[2]
        n2 = a[0] * b[1] - a[1] * b[0]
        sine = jnp.sqrt(n0 * n0 + n1 * n1 + n2 * n2)
        cosine = a[0] * b[0] + a[1] * b[1] + a[2] * b[2]
        angle = jnp.arctan2(sine, cosine)
        return angle * angle

    def distances(z, acc):
        p = [prior[c, z] for c in range(3)]
        a = [m[0, c, z] for c in range(3)]
        b = [m[1, c, z] for c in range(3)]
        n = [nxt[c, z] for c in range(3)]
        return (
            acc[0] + angle_squared(a, p),
            acc[1] + angle_squared(a, b),
            acc[2] + angle_squared(b, n),
        )

    flat = jnp.zeros((NROW, NY), F32)
    spans = [total(x) for x in lax.fori_loop(0, NZ, distances, (flat, flat, flat))]

    mine = got_e.at[1, pl.ds(0, SPACE - 1)]
    wait_bytes(mine, e_r)
    for present, group, slot in ((has_prior, 0, 0), (has_next, 2, 1)):
        @pl.when(present)
        def _(group=group, slot=slot):
            wait_bytes(got_e.at[group], n_r.at[slot])

        @pl.when(jnp.logical_not(present))
        def _(group=group):
            got_e[group] = got_e[1]

    e_prior, e_own, e_next = (-0.5 * sum_round(got_e.at[g]) for g in range(3))
    tile_x[0] = e_own / CELLS

    line = [e_prior[0:1, 1:2], e_own[0:1, 0:1], e_own[0:1, 1:2], e_next[0:1, 0:1]]
    lengths = []
    for i in range(2):
        rise_next = line[i + 2] - line[i + 1]
        rise_prior = line[i + 1] - line[i]
        upward = (rise_next > 0) & (rise_prior > 0)
        downward = (rise_next < 0) & (rise_prior < 0)
        larger = jnp.maximum(jnp.abs(rise_next), jnp.abs(rise_prior))
        smaller = jnp.minimum(jnp.abs(rise_next), jnp.abs(rise_prior))
        toward_next = line[i + 2] > line[i]
        one, nil = jnp.ones((1, 1), F32), jnp.zeros((1, 1), F32)
        w_next = jnp.where(
            upward, one, jnp.where(downward, nil, jnp.where(toward_next, larger, smaller))
        )
        w_prior = jnp.where(
            upward, nil, jnp.where(downward, one, jnp.where(toward_next, smaller, larger))
        )
        w_next = jnp.broadcast_to(w_next, (NROW, NY))
        w_prior = jnp.broadcast_to(w_prior, (NROW, NY))

        def tangent(z, acc, i=i, w_next=w_next, w_prior=w_prior):
            own = [m[i, c, z] for c in range(3)]
            ahead = [m[1, c, z] if i == 0 else nxt[c, z] for c in range(3)]
            behind = [prior[c, z] if i == 0 else m[0, c, z] for c in range(3)]
            v = [
                w_next * (ahead[c] - own[c]) + w_prior * (own[c] - behind[c]) for c in range(3)
            ]
            along = v[0] * own[0] + v[1] * own[1] + v[2] * own[2]
            for c in range(3):
                t = v[c] - along * own[c]
                tang[i, c, z] = t
                acc = acc + t * t
            return acc

        lengths.append(total(lax.fori_loop(0, NZ, tangent, flat)))

    for t in range(2):
        @pl.when(me != (1 - t) * NZ)
        def _(t=t):
            wait_bytes(hbuf.at[t], g_r.at[t])

    def add_halves(image, c, sign, values):
        for n in range(NZ // 2):
            floc[image, c, n] = floc[image, c, n] + values[n]
            floc[image, c, NZ - 1 - n] = floc[image, c, NZ - 1 - n] + sign * values[n]

    def own_result(j):
        sign = jnp.where(part_of(j) == 0, 1.0, -1.0)
        c = j % 3

        def put(n, value):
            floc[hi, c, n] = floc[hi, c, n] + value
            floc[hi, c, NZ - 1 - n] = floc[hi, c, NZ - 1 - n] + sign * value

        half_layers(0, j, put)
        result_copy(j).wait_recv()
        add_halves(1 - hi, c, sign, [rbuf[j, n] for n in range(NZ // 2)])

    def extra_result(c):
        add_halves(0, c, -1.0, [hbuf[0, c] * layer_wave(NZ, n, True) for n in range(NZ // 2)])
        add_halves(1, c, 1.0, [hbuf[1, c] * layer_wave(0, n, False) for n in range(NZ // 2)])

    each(0, 3, extra_result)
    each(0, 6, own_result)

    drives = []
    for i in range(2):
        def force(z, acc, i=i):
            own = [m[i, c, z] for c in range(3)]
            f = [floc[i, c, z] for c in range(3)]
            along = f[0] * own[0] + f[1] * own[1] + f[2] * own[2]
            for c in range(3):
                t = f[c] - along * own[c]
                floc[i, c, z] = t
                acc = acc + t * tang[i, c, z]
            return acc

        drives.append(total(lax.fori_loop(0, NZ, force, flat)))

    send_round(round_c, msg_c, got_c, line_of(lengths + drives + spans))
    round_c[1]()
    sums = sum_round(got_c)
    dist = [jnp.sqrt(sums[0:1, 4 + j : 5 + j] / CELLS) for j in range(3)]
    tops = []
    for i in range(2):
        scale = jnp.sqrt(sums[0:1, i : i + 1] / CELLS + epsilon)
        parallel = sums[0:1, 2 + i : 3 + i] / (CELLS * scale)
        spring = spring_strength * (dist[i + 1] - dist[i])
        index = 2 * im + i
        interior = (index > 0) & (index < 2 * images - 1)
        coef = jnp.broadcast_to((spring - parallel) / scale, (NROW, NY))
        inner = jnp.where(interior, 1, 0)

        def band(z, acc, i=i, coef=coef, inner=inner):
            size = None
            for c in range(3):
                b = floc[i, c, z] + coef * tang[i, c, z]
                b = jnp.where(inner > 0, b, 0.0)
                out_b[i, c, z] = b
                size = b * b if size is None else size + b * b
            return jnp.maximum(acc, size)

        top = lax.fori_loop(0, NZ, band, flat)
        tops.append(jnp.max(jnp.max(top, axis=0, keepdims=True), axis=1, keepdims=True))

    send_round(round_d, msg_d, got_d, line_of(tops))
    round_d[1]()
    largest = got_d[0]
    for s in range(1, SPACE):
        largest = jnp.maximum(largest, got_d[s])
    largest = jnp.sqrt(largest)
    tile_x[1] = largest

    def drain(k):
        @pl.when(near(k) % NZ != 0)
        def _():
            wait_bytes(sbuf.at[0, pl.ds(0, 2)], y_s.at[k])

        @pl.when(near(k) % NZ == 0)
        def _():
            wait_bytes(sbuf.at[0, 0], y_s.at[k])

        @pl.when(special)
        def _():
            wait_bytes(sbuf.at[0, 0], f_s.at[k])

        @pl.when(jnp.logical_not(special))
        def _():
            wait_bytes(sbuf.at[0, pl.ds(0, 2)], f_s.at[k])

    each(1, NZ, drain)

    @pl.when(special)
    def _():
        wait_bytes(fbuf.at[pl.ds(0, 3), pl.ds(0, SPACE - 1)], g_s)

    for t in range(2):
        @pl.when(me != t * NZ)
        def _(t=t):
            wait_bytes(xbuf.at[t], x_s.at[t])

    each(0, 3, lambda c: partner_copy(c).wait_send())
    each(0, 6, lambda j: result_copy(j).wait_send())
    for rnd in (round_c, round_d):
        rnd[2]()
    wait_bytes(mine, e_s)
    at_images(lambda other, slot: wait_bytes(got_e.at[2 * slot], n_s.at[slot]))
    at_images(lambda other, slot: image_copy(other, slot).wait_send())
    at_slabs(lambda side: halo_copy(side).wait_send())


def finish_kernel(m_ref, b_ref, tile_ref, upd_hbm, bf_hbm, en_ref, upd, sem):
    stores = [pltpu.make_async_copy(b_ref, bf_hbm, sem.at[2])]
    stores[0].start()
    for i in range(2):
        en_ref[i] = jnp.max(tile_ref[0, :, i : i + 1])
        move = jnp.minimum(
            step_limit, rotation_limit / (tile_ref[1, :, i : i + 1] + epsilon)
        )
        move = jnp.broadcast_to(move, (NROW, NY))

        def advance(z, carry, i=i, move=move):
            s = [m_ref[i, c, z] + move * b_ref[i, c, z] for c in range(3)]
            length = jnp.sqrt(s[0] * s[0] + s[1] * s[1] + s[2] * s[2])
            for c in range(3):
                upd[i, c, z] = s[c] / length
            return carry

        lax.fori_loop(0, NZ, advance, 0)
        stores.append(pltpu.make_async_copy(upd.at[i], upd_hbm.at[i], sem.at[i]))
        stores[-1].start()
    for c in stores:
        c.wait()


def body(magnet, anisotropy, kernel):
    table = wave_table(NX)
    across = np.concatenate(split_table(np.ascontiguousarray(table.T)), axis=1)
    tables = jnp.asarray(np.concatenate([*split_table(table), across], axis=0))
    slab = (2, 3, NZ, NROW, NY)
    vm = pltpu.VMEM
    dma = pltpu.SemaphoreType.DMA
    tile = (1, 128)
    scratch = [
        vm(slab[1:], F32), vm(slab[1:], F32),
        vm((2, 2, 3, NZ, NY), F32), vm((2, 2, 3, NZ, NY), F32),
        vm(slab[1:], F32), vm((2, 3, NROW, NY), F32),
        vm((2, NZ, 6, NROW, NY), F32), vm((6, SPACE, NROW, NY), F32),
        vm((NX, 2 * NY), BF16), vm((NX, 2 * NY), BF16),
        vm((6, 2 * NX, 2 * NY), F32),
        vm((6, 2 * NX, 2 * NY), BF16), vm((6, 2 * NX, 2 * NY), BF16),
        vm((6, NX + 8, NY + 128), F32), vm((6, 2 * NX, 2 * NY), F32),
        vm((NX, 2 * NY), BF16), vm((NX, 2 * NY), BF16),
        vm((6, SPACE, NROW, NY), F32), vm((2, 6, NZ, NROW, NY), F32),
        vm((6, NZ // 2, NROW, NY), F32), vm((6, NZ // 2, NROW, NY), F32), vm((2, 3, NROW, NY), F32),
        vm(slab, F32), vm(slab, F32),
        vm((2 * NX, 2 * NY), BF16), vm((2, 2 * NX, NY), BF16), pltpu.SMEM((NROW,), F32),
        vm(tile, F32), vm((3, SPACE, *tile), F32),
        vm(tile, F32), vm((SPACE, *tile), F32),
        vm(tile, F32), vm((SPACE, *tile), F32),
        dma((6,)),
        dma((3,)), dma((3,)), dma((2,)), dma((3,)),
        dma((NZ,)), dma((6,)), dma((NZ,)), dma((2, 6)), dma, dma((2,)), dma((6,)), dma((6,)),
        dma, dma, dma((2,)), dma((2,)), dma, dma, dma, dma,
        dma((2,)), dma((2,)), dma((2,)), dma((2,)),
    ]
    hbm = pl.BlockSpec(memory_space=pltpu.HBM)
    vmem = pl.BlockSpec(memory_space=pltpu.VMEM)
    smem = pl.BlockSpec(memory_space=pltpu.SMEM)
    own, band, tiles = pl.pallas_call(
        step_kernel,
        out_shape=(
            jax.ShapeDtypeStruct(slab, F32),
            jax.ShapeDtypeStruct(slab, F32),
            jax.ShapeDtypeStruct((2, *tile), F32),
        ),
        in_specs=[hbm] * 4,
        out_specs=(vmem, vmem, vmem),
        scratch_shapes=scratch,
        compiler_params=pltpu.CompilerParams(
            collective_id=0, has_side_effects=True, vmem_limit_bytes=STEP_VMEM
        ),
        name="band_step",
    )(magnet, anisotropy, kernel, tables)
    return pl.pallas_call(
        finish_kernel,
        out_shape=(
            jax.ShapeDtypeStruct(slab, F32),
            jax.ShapeDtypeStruct(slab, F32),
            jax.ShapeDtypeStruct((2,), F32),
        ),
        in_specs=[vmem, vmem, vmem],
        out_specs=(hbm, hbm, smem),
        scratch_shapes=[vm(slab, F32), dma((3,))],
        compiler_params=pltpu.CompilerParams(vmem_limit_bytes=3 * 2**20),
        name="band_finish",
    )(own, band, tiles)


def solution(mesh):
    in_specs = (P("image", None, None, "space", None), P("space"), P(None, "space", None, None))
    out_specs = (
        P("image", None, None, "space", None),
        P("image", None, None, "space", None),
        P("image"),
    )
    return jax.shard_map(body, mesh=mesh, in_specs=in_specs, out_specs=out_specs, check_vma=False)
```

```python
import math

import jax
import jax.numpy as jnp
import numpy as np
from jax import lax
from jax.experimental import pallas as pl
from jax.experimental.pallas import tpu as pltpu
from jax.sharding import PartitionSpec as P

F32 = jnp.float32
BF16 = jnp.bfloat16
MESH = pl.DeviceIdType.MESH

exchange_strength = 0.25
chiral_strength = 0.3
spring_strength = 10.0
step_limit = 1.0
rotation_limit = 0.5
epsilon = 1e-06

NZ, NROW, NY, NX = 8, 16, 256, 256
SPACE = 16
CELLS = NZ * NX * NY
STEP_VMEM = 53200 * 1024


def split_table(table):
    high = table.astype(np.dtype(BF16))
    low = (table - high.astype(np.float64)).astype(np.dtype(BF16))
    return high, low


def wave_table(count):
    position = 2 * np.arange(count)[:, None] - (count - 1)
    cosine = np.arange(count)[None, :]
    sine = np.where(cosine == 0, count, cosine)
    unit = 2.0 * math.pi / (4 * count)
    return np.concatenate(
        [
            np.cos((cosine * position % (4 * count)) * unit),
            np.sin((sine * position % (4 * count)) * unit),
        ],
        axis=1,
    )


def layer_wave(q, n, sine):
    angle = 2.0 * math.pi * q * (n - (NZ - 1) / 2) / (2 * NZ)
    return float(math.sin(angle) if sine else math.cos(angle))


def split(x):
    high = x.astype(BF16)
    low = (x - high.astype(F32)).astype(BF16)
    return high, low


def mm(a, b):
    return jnp.dot(a, b, preferred_element_type=F32)


def total(x):
    return jnp.sum(jnp.sum(x, axis=0, keepdims=True), axis=1, keepdims=True)


def line_of(values):
    lane = lax.broadcasted_iota(jnp.int32, (1, 128), 1)
    line = jnp.zeros((1, 128), F32)
    for j, v in enumerate(values):
        line = jnp.where(lane == j, v, line)
    return line


def step_kernel(
    m_hbm, ani_hbm, k_hbm, tab_hbm,
    m, out_b, tile_x,
    prior, nxt, halo_out, halo_in, ebuf, pbuf, xbuf, sbuf, ybuf, zhi, zlo, spec, rhi, rlo,
    kraw, keff, uboth, fbuf, gbuf, obuf, rbuf, hbuf, floc, tang,
    wtab, ttab, ani_ref,
    msg_e, got_e, msg_c, got_c, msg_d, got_d,
    in_sem, p_s, p_r, x_s, x_r, y_s, y_r, f_s, f_r, g_s, g_r, o_s, o_r,
    e_s, e_r, n_s, n_r, c_s, c_r, d_s, d_r, i_s, i_r, h_s, h_r,
):
    im = lax.axis_index("image")
    me = lax.axis_index("space")
    images = lax.axis_size("image")
    hi, spot = me // NZ, me % NZ
    partner = (1 - hi) * NZ + spot
    special = spot == 0

    def dest(k):
        return (me + k) % SPACE

    def piece(c, part):
        if isinstance(c, int):
            return 3 * (1 - part if c == 2 else part) + c
        return 3 * jnp.where(c == 2, 1 - part, part) + c

    def part_of(j):
        return jnp.where(j % 3 == 2, 1 - j // 3, j // 3)

    def is_regular(j):
        return jnp.logical_not(special) | (part_of(j) == hi)

    def near(k):
        return hi * NZ + (spot + k) % NZ

    def each(lo, up, do):
        lax.fori_loop(lo, up, lambda k, x: (do(k), x)[1], 0)

    def remote(src, dst, send, recv, device):
        return pltpu.make_async_remote_copy(
            src_ref=src, dst_ref=dst, send_sem=send, recv_sem=recv,
            device_id={"space": device}, device_id_type=MESH,
        )

    def wait_bytes(ref, sem):
        pltpu.make_async_copy(ref, ref, sem).wait()

    def plane_sides(h):
        rows = [(0, h, h == 1, NZ * h)]
        for t in range(1, NZ):
            rows += [(t, 0, False, NZ * h + t), (t, 1, True, NZ * h + t)]
        return rows

    def layer_sums(lines):
        half = NZ // 2
        even = [lines[n] + lines[NZ - 1 - n] for n in range(half)]
        odd = [lines[n] - lines[NZ - 1 - n] for n in range(half)]
        return even, odd

    def layer_dot(terms, q, sine):
        acc = terms[0] * layer_wave(q, 0, sine)
        for n in range(1, NZ // 2):
            acc = acc + terms[n] * layer_wave(q, n, sine)
        return acc

    has_next, has_prior = im < images - 1, im > 0
    im_next = jnp.minimum(im + 1, images - 1)
    im_prior = jnp.maximum(im - 1, 0)
    sp_next = jnp.minimum(me + 1, SPACE - 1)
    sp_prior = jnp.maximum(me - 1, 0)

    loads = [
        pltpu.make_async_copy(tab_hbm.at[pl.ds(0, 2 * NX)], wtab, in_sem.at[0]),
        pltpu.make_async_copy(
            tab_hbm.at[pl.ds(2 * NX, 2 * NX), pl.ds(0, NY)], ttab.at[0], in_sem.at[1]
        ),
        pltpu.make_async_copy(
            tab_hbm.at[pl.ds(2 * NX, 2 * NX), pl.ds(NY, NY)], ttab.at[1], in_sem.at[2]
        ),
        pltpu.make_async_copy(ani_hbm, ani_ref, in_sem.at[3]),
        pltpu.make_async_copy(
            k_hbm.at[:, 0, pl.ds(0, NX + 8), pl.ds(0, NY + 128)], kraw, in_sem.at[4]
        ),
    ]
    load_m = pltpu.make_async_copy(m_hbm, m, in_sem.at[5])
    load_m.start()
    for c in loads:
        c.start()
    whi, wlo = wtab.at[pl.ds(0, NX)], wtab.at[pl.ds(NX, NX)]
    thi, tlo = ttab.at[0], ttab.at[1]

    barrier = pltpu.get_barrier_semaphore()

    def greet(k, carry):
        pl.semaphore_signal(barrier, inc=1, device_id={"space": dest(k)}, device_id_type=MESH)
        return carry

    lax.fori_loop(1, SPACE, greet, 0)

    def at_images(do):
        for present, other, slot in ((has_next, im_next, 0), (has_prior, im_prior, 1)):
            @pl.when(present)
            def _(other=other, slot=slot):
                do(other, slot)

    at_images(
        lambda other, slot: each(
            0, SPACE,
            lambda k: pl.semaphore_signal(
                barrier, inc=1, device_id={"image": other, "space": k}, device_id_type=MESH
            ),
        )
    )
    greeted = SPACE - 1 + SPACE * (jnp.minimum(im, 1) + jnp.minimum(images - 1 - im, 1))

    load_m.wait()
    def own_layers(c):
        for h in range(2):
            @pl.when(hi == h)
            def _(h=h):
                even, odd = layer_sums([m[h, c, n] for n in range(NZ)])
                for t, part, sine, q in plane_sides(h):
                    sbuf[0, t, piece(c, part)] = layer_dot(odd if sine else even, q, sine)
                other_even, other_odd = layer_sums([m[1 - h, c, n] for n in range(NZ)])
                for n in range(NZ // 2):
                    ebuf[piece(c, 0), n] = other_even[n]
                    ebuf[piece(c, 1), n] = other_odd[n]
                xbuf[0, c] = layer_dot(even if h == 1 else other_even, 0, False)
                xbuf[1, c] = layer_dot(odd if h == 0 else other_odd, NZ, True)

    each(0, 3, own_layers)

    for i in range(2):
        for c in range(3):
            halo_out[0, i, c] = m[i, c, :, 0, :]
            halo_out[1, i, c] = m[i, c, :, NROW - 1, :]

    pl.semaphore_wait(barrier, greeted)

    def partner_copy(j):
        return remote(ebuf.at[j], pbuf.at[j], p_s.at[j], p_r.at[j], partner)

    def plane_copy(u, j, k):
        to = near(k)
        slab = me if u == 0 else partner
        return remote(
            sbuf.at[u, to % NZ, j], ybuf.at[j, slab], y_s.at[k], y_r.at[j], to
        )

    def extra_copy(t, c):
        return remote(
            xbuf.at[t, c], ybuf.at[piece(c, 1 - t), me], x_s.at[t], x_r.at[c], t * NZ
        )

    def send_planes(u, first, last):
        def one(j):
            def to(k):
                @pl.when((near(k) % NZ != 0) | (part_of(j) == hi))
                def _():
                    plane_copy(u, j, k).start()

            each(1, NZ, to)

            @pl.when(is_regular(j))
            def _():
                slab = me if u == 0 else partner
                ybuf[j, pl.ds(slab, 1)] = sbuf[u, spot, pl.ds(j, 1)]

        each(first, last, one)

    def halo_copy(side):
        return remote(
            halo_out.at[side], halo_in.at[1 - side], h_s.at[side], h_r.at[side],
            (sp_prior, sp_next)[side],
        )

    def at_slabs(do):
        for side, present in ((0, me > 0), (1, me < SPACE - 1)):
            @pl.when(present)
            def _(side=side):
                do(side)

    def image_copy(other, slot):
        return pltpu.make_async_remote_copy(
            src_ref=m.at[1 - slot], dst_ref=(prior, nxt)[slot], send_sem=i_s.at[slot],
            recv_sem=i_r.at[slot], device_id={"image": other}, device_id_type=MESH,
        )

    at_slabs(lambda side: halo_copy(side).start())
    for t in range(2):
        @pl.when(me != t * NZ)
        def _(t=t):
            each(0, 3, lambda c: extra_copy(t, c).start())

        @pl.when(me == t * NZ)
        def _(t=t):
            for c in range(3):
                ybuf[piece(c, 1 - t), pl.ds(me, 1)] = xbuf[t, pl.ds(c, 1)]

    each(0, 3, lambda j: partner_copy(j).start())
    send_planes(0, 0, 3)
    each(3, 6, lambda j: partner_copy(j).start())

    loads[4].wait()
    plane_weight = jnp.where(me % NZ == 0, 1.0, 2.0) * (-4.0 / (2 * NZ * 2 * NX * 2 * NY))
    lane = lax.broadcasted_iota(jnp.int32, (64, 128), 1)

    def prepare(t, carry):
        comp, first = t // 4, pl.multiple_of((t % 4) * 64, 64)
        row = lax.broadcasted_iota(jnp.int32, (64, NY), 0) + first
        column = lax.broadcasted_iota(jnp.int32, (64, NY), 1)
        weight = plane_weight * jnp.where(row == 0, 0.5, 1.0) * jnp.where(column == 0, 0.5, 1.0)
        base = kraw[comp, pl.ds(first, 64), pl.ds(0, NY)]
        edge = kraw[comp, pl.ds(first, 64), pl.ds(NY, 128)]
        last = kraw[comp, pl.ds(NX, 8), pl.ds(0, NY)][0:1]
        last_edge = kraw[comp, pl.ds(NX, 8), pl.ds(NY, 128)][0:1]
        top = row == 0
        for bx in range(2):
            body_part = jnp.where(top, last, base) if bx else base
            edge_part = jnp.where(top[:, :128], last_edge, edge) if bx else edge
            for by in range(2):
                if by:
                    left = jnp.where(lane == 0, edge_part, body_part[:, :128])
                    value = jnp.concatenate([left, body_part[:, 128:]], axis=1)
                else:
                    value = body_part
                keff[comp, pl.ds(bx * NX + first, 64), pl.ds(by * NY, NY)] = value * weight
        return carry

    lax.fori_loop(0, 24, prepare, 0)

    def partner_layers(j):
        partner_copy(j).wait_recv()
        terms = [pbuf[j, n] for n in range(NZ // 2)]
        for h in range(2):
            for part in range(2):
                @pl.when((hi == h) & (part_of(j) == part))
                def _(h=h, part=part):
                    for t, own_part, sine, q in plane_sides(h):
                        if own_part == part:
                            sbuf[1, t, j] = layer_dot(terms, q, sine)

        send_planes(1, j, j + 1)

    each(0, 3, partner_layers)
    send_planes(0, 3, 6)

    @pl.when(me < SPACE - 1)
    def _():
        halo_copy(0).wait_recv()

    @pl.when(me > 0)
    def _():
        halo_copy(1).wait_recv()

    row = lax.broadcasted_iota(jnp.int32, (NROW, NY), 0)
    column = lax.broadcasted_iota(jnp.int32, (NROW, NY), 1)
    loads[3].wait()
    easy = jnp.zeros((NROW, NY), F32)
    for r in range(NROW):
        easy = jnp.where(row == r, 2.0 * ani_ref[r], easy)
    edges = (
        jnp.where((row == 0) & (me == 0), 1.0, 0.0)
        + jnp.where((row == NROW - 1) & (me == SPACE - 1), 1.0, 0.0)
        + jnp.where(column == 0, 1.0, 0.0)
        + jnp.where(column == NY - 1, 1.0, 0.0)
    )

    def local_part(i):
        def layer(z, acc):
            at_bottom = z == 0
            at_top = z == NZ - 1
            present = 6.0 - edges - jnp.where(at_bottom | at_top, 1.0, 0.0)
            own, xp, xm, yp, ym, field = [], [], [], [], [], []
            for c in range(3):
                v = m[i, c, z]
                before = jnp.where(me == 0, 0.0, halo_in[0, i, c, pl.ds(z, 1), :])
                after = jnp.where(me == SPACE - 1, 0.0, halo_in[1, i, c, pl.ds(z, 1), :])
                own.append(v)
                xp.append(jnp.where(row == NROW - 1, after, pltpu.roll(v, NROW - 1, 0)))
                xm.append(jnp.where(row == 0, before, pltpu.roll(v, 1, 0)))
                yp.append(jnp.where(column == NY - 1, 0.0, pltpu.roll(v, NY - 1, 1)))
                ym.append(jnp.where(column == 0, 0.0, pltpu.roll(v, 1, 1)))
                zp = jnp.where(at_top, 0.0, m[i, c, jnp.minimum(z + 1, NZ - 1)])
                zm = jnp.where(at_bottom, 0.0, m[i, c, jnp.maximum(z - 1, 0)])
                around = xp[c] + xm[c] + yp[c] + ym[c] + zp + zm
                field.append(exchange_strength * (around - present * v))
            field[0] = field[0] + chiral_strength * (xp[2] - xm[2])
            field[1] = field[1] + chiral_strength * (yp[2] - ym[2])
            field[2] = (
                field[2]
                - chiral_strength * ((xp[0] - xm[0]) + (yp[1] - ym[1]))
                + easy * own[2]
            )
            for c in range(3):
                floc[i, c, z] = field[c]
                acc = acc + field[c] * own[c]
            return acc

        return lax.fori_loop(0, NZ, layer, jnp.zeros((NROW, NY), F32))

    local_energy = [total(local_part(0))]
    local_energy.append(total(local_part(1)))
    each(3, 6, partner_layers)
    at_images(lambda other, slot: image_copy(other, slot).start())

    for c in loads[0:3]:
        c.wait()

    def forward(j, carry):
        regular = is_regular(j)

        @pl.when(regular)
        def _():
            wait_bytes(ybuf.at[j, pl.ds(0, SPACE - 2)], y_r.at[j])

        @pl.when(jnp.logical_not(regular))
        def _():
            wait_bytes(ybuf.at[j, pl.ds(0, SPACE - 1)], x_r.at[j % 3])

        high, low = split(ybuf[j].reshape(NX, NY))
        stacked = jnp.concatenate([high, low], axis=0)
        for n in range(2):
            ns = pl.ds(n * NY, NY)
            both = mm(stacked, whi[:, ns])
            out = both[:NX] + mm(high, wlo[:, ns]) + both[NX:]
            zhi[:, ns], zlo[:, ns] = split(out)
        for n in range(2):
            ns = pl.ds(n * NY, NY)
            zh, zl = zhi[:, ns], zlo[:, ns]
            spec[j, :, ns] = mm(thi[...], zh) + mm(tlo[...], zh) + mm(thi[...], zl)
        return carry

    def respond(g):
        def block(t, acc):
            for half in range(2):
                acc = quarter(pl.multiple_of(t * 16, 16), half * 128, acc)
            return acc

        def quarter(r0, l0, acc):
            def at(bx, by):
                return (pl.ds(bx * NX + r0, 16), pl.ds(by * NY + l0, 128))

            parts = (g, g, 1 - g)
            v = {
                (c, bx, by): spec[(3 * g + c, *at(bx, by))]
                for c in range(3) for bx in range(2) for by in range(2)
            }
            sums = list(acc)

            def plus(x, minus, y):
                return x - y if minus else x + y

            for bx in range(2):
                for by in range(2):
                    here = at(bx, by)
                    k = [keff[(comp, *here)] for comp in range(6)]
                    fx = plus(k[0] * v[0, bx, by], bx == by, k[3] * v[1, 1 - bx, 1 - by])
                    fx = plus(fx, parts[0] == bx, k[4] * v[2, 1 - bx, by])
                    fy = plus(k[1] * v[1, bx, by], bx == by, k[3] * v[0, 1 - bx, 1 - by])
                    fy = plus(fy, parts[1] == by, k[5] * v[2, bx, 1 - by])
                    fz = plus(k[2] * v[2, bx, by], parts[2] == bx, k[4] * v[0, 1 - bx, by])
                    fz = plus(fz, parts[2] == by, k[5] * v[1, bx, 1 - by])
                    sums[0] = sums[0] + (fx * v[0, bx, by] + fy * v[1, bx, by])
                    sums[1] = sums[1] + fz * v[2, bx, by]
                    for c, f in enumerate((fx, fy, fz)):
                        rhi[(3 * g + c, *here)], rlo[(3 * g + c, *here)] = split(f)
            return tuple(sums)

        zero = jnp.zeros((16, 128), F32)
        flat_sum, z_sum = lax.fori_loop(0, 16, block, (zero, zero))
        return (flat_sum, z_sum) if g == 0 else (z_sum, flat_sum)

    def small_round(msg, got, s_sem, r_sem):
        def copy(k):
            return pltpu.make_async_remote_copy(
                src_ref=msg, dst_ref=got.at[me], send_sem=s_sem,
                recv_sem=r_sem, device_id={"space": dest(k)}, device_id_type=MESH,
            )

        part = got.at[pl.ds(0, SPACE - 1)]

        def start():
            lax.fori_loop(1, SPACE, lambda k, x: (copy(k).start(), x)[1], 0)

        def finish():
            pltpu.make_async_copy(part, part, r_sem).wait()

        def drain():
            pltpu.make_async_copy(part, part, s_sem).wait()

        return start, finish, drain

    def send_round(rnd, msg, got, tile):
        msg[...] = tile
        got[me] = tile
        rnd[0]()

    def sum_round(got):
        acc = got[0]
        for s in range(1, SPACE):
            acc = acc + got[s]
        return acc

    round_c = small_round(msg_c, got_c, c_s, c_r)
    round_d = small_round(msg_d, got_d, d_s, d_r)

    def energy_copy(k):
        return pltpu.make_async_remote_copy(
            src_ref=msg_e, dst_ref=got_e.at[1, me], send_sem=e_s,
            recv_sem=e_r, device_id={"space": dest(k)}, device_id_type=MESH,
        )

    def image_energy_copy(other, slot, k):
        return pltpu.make_async_remote_copy(
            src_ref=msg_e, dst_ref=got_e.at[2 * slot, me], send_sem=n_s.at[slot],
            recv_sem=n_r.at[slot], device_id={"image": other, "space": k},
            device_id_type=MESH,
        )

    def field_copy(u, j, k):
        to = near(k)
        slab = to if u == 0 else (1 - hi) * NZ + to % NZ
        return remote(
            fbuf.at[j, slab], gbuf.at[u, j, spot], f_s.at[k], f_r.at[u, j], to
        )

    def return_copy(c, k):
        part = 1 - hi
        to = dest(k)
        return remote(
            fbuf.at[piece(c, part), to], hbuf.at[1 - hi, c], g_s, g_r.at[1 - hi], to
        )

    def send_fields(u, j):
        @pl.when(is_regular(j))
        def _():
            each(1, NZ, lambda k: field_copy(u, j, k).start())
            slab = me if u == 0 else partner
            gbuf[u, j, pl.ds(spot, 1)] = fbuf[j, pl.ds(slab, 1)]

    def backward(j, carry):
        for n in range(2):
            ns = pl.ds(n * NY, NY)
            rh, rl = rhi[j, :, ns], rlo[j, :, ns]
            both = mm(wtab[...], rh)
            u = both[:NX] + both[NX:] + mm(whi[...], rl)
            uboth[:NX, ns], uboth[NX:, ns] = split(u)
        both = mm(uboth[...], thi[...])
        f = both[:NX] + mm(uboth[:NX], tlo[...]) + both[NX:]
        fbuf[j] = f.reshape(SPACE, NROW, NY)
        send_fields(1, j)

        @pl.when(jnp.logical_not(is_regular(j)))
        def _():
            each(1, SPACE, lambda k: return_copy(j % 3, k).start())
            hbuf[1 - hi, pl.ds(j % 3, 1)] = fbuf[j, pl.ds(me, 1)]

        return carry

    def wait_fields(u, j):
        full = special | (part_of(j) == hi)

        @pl.when(full)
        def _():
            wait_bytes(gbuf.at[u, j, pl.ds(0, NZ - 1)], f_r.at[u, j])

        @pl.when(jnp.logical_not(full))
        def _():
            wait_bytes(gbuf.at[u, j, pl.ds(0, NZ - 2)], f_r.at[u, j])

    def half_layers(u, j, put):
        wait_fields(u, j)
        for h in range(2):
            for part in range(2):
                @pl.when((hi == h) & (part_of(j) == part))
                def _(h=h, part=part):
                    sums = [None] * (NZ // 2)
                    for t, own_part, sine, q in plane_sides(h):
                        if own_part != part:
                            continue
                        v = gbuf[u, j, t]
                        for n in range(NZ // 2):
                            term = v * layer_wave(q, n, sine)
                            sums[n] = term if sums[n] is None else sums[n] + term
                    for n in range(NZ // 2):
                        put(n, sums[n])

    def result_copy(j):
        return remote(obuf.at[j], rbuf.at[j], o_s.at[j], o_r.at[j], partner)

    def partner_result(j):
        def put(n, value):
            obuf[j, n] = value

        half_layers(1, j, put)
        result_copy(j).start()

    lax.fori_loop(0, 3, forward, 0)
    first_a, first_b = respond(0)
    lax.fori_loop(0, 3, backward, 0)
    each(0, 3, lambda j: send_fields(0, j))
    lax.fori_loop(3, 6, forward, 0)
    second_a, second_b = respond(1)
    part_a, part_b = total(first_a + second_a), total(first_b + second_b)
    none = jnp.zeros((1, 1), F32)
    first_share = jnp.where(me <= NZ, part_a, none) + jnp.where(
        (me >= 1) & (me < NZ), part_b, none
    )
    second_share = jnp.where(me > NZ, part_a, none) + jnp.where(
        (me == 0) | (me >= NZ), part_b, none
    )
    line = line_of([local_energy[0] + first_share, local_energy[1] + second_share])
    msg_e[...] = line
    got_e[1, me] = line
    lax.fori_loop(1, SPACE, lambda k, x: (energy_copy(SPACE - k).start(), x)[1], 0)
    at_images(
        lambda other, slot: each(
            0, SPACE, lambda k: image_energy_copy(other, slot, k).start()
        )
    )

    each(0, 3, partner_result)
    lax.fori_loop(3, 4, backward, 0)
    lax.fori_loop(4, 6, backward, 0)
    each(3, 6, lambda j: send_fields(0, j))

    each(3, 6, partner_result)

    @pl.when(has_prior)
    def _():
        image_copy(im_next, 0).wait_recv()

    @pl.when(has_next)
    def _():
        image_copy(im_prior, 1).wait_recv()

    @pl.when(jnp.logical_not(has_prior))
    def _():
        prior[...] = m[0]

    @pl.when(jnp.logical_not(has_next))
    def _():
        nxt[...] = m[1]


    def angle_squared(a, b):
        n0 = a[1] * b[2] - a[2] * b[1]
        n1 = a[2] * b[0] - a[0] * b[2]
        n2 = a[0] * b[1] - a[1] * b[0]
        sine = jnp.sqrt(n0 * n0 + n1 * n1 + n2 * n2)
        cosine = a[0] * b[0] + a[1] * b[1] + a[2] * b[2]
        angle = jnp.arctan2(sine, cosine)
        return angle * angle

    def distances(z, acc):
        p = [prior[c, z] for c in range(3)]
        a = [m[0, c, z] for c in range(3)]
        b = [m[1, c, z] for c in range(3)]
        n = [nxt[c, z] for c in range(3)]
        return (
            acc[0] + angle_squared(a, p),
            acc[1] + angle_squared(a, b),
            acc[2] + angle_squared(b, n),
        )

    flat = jnp.zeros((NROW, NY), F32)
    spans = [total(x) for x in lax.fori_loop(0, NZ, distances, (flat, flat, flat))]

    mine = got_e.at[1, pl.ds(0, SPACE - 1)]
    wait_bytes(mine, e_r)
    for present, group, slot in ((has_prior, 0, 0), (has_next, 2, 1)):
        @pl.when(present)
        def _(group=group, slot=slot):
            wait_bytes(got_e.at[group], n_r.at[slot])

        @pl.when(jnp.logical_not(present))
        def _(group=group):
            got_e[group] = got_e[1]

    e_prior, e_own, e_next = (-0.5 * sum_round(got_e.at[g]) for g in range(3))
    tile_x[0] = e_own / CELLS

    line = [e_prior[0:1, 1:2], e_own[0:1, 0:1], e_own[0:1, 1:2], e_next[0:1, 0:1]]
    lengths = []
    for i in range(2):
        rise_next = line[i + 2] - line[i + 1]
        rise_prior = line[i + 1] - line[i]
        upward = (rise_next > 0) & (rise_prior > 0)
        downward = (rise_next < 0) & (rise_prior < 0)
        larger = jnp.maximum(jnp.abs(rise_next), jnp.abs(rise_prior))
        smaller = jnp.minimum(jnp.abs(rise_next), jnp.abs(rise_prior))
        toward_next = line[i + 2] > line[i]
        one, nil = jnp.ones((1, 1), F32), jnp.zeros((1, 1), F32)
        w_next = jnp.where(
            upward, one, jnp.where(downward, nil, jnp.where(toward_next, larger, smaller))
        )
        w_prior = jnp.where(
            upward, nil, jnp.where(downward, one, jnp.where(toward_next, smaller, larger))
        )
        w_next = jnp.broadcast_to(w_next, (NROW, NY))
        w_prior = jnp.broadcast_to(w_prior, (NROW, NY))

        def tangent(z, acc, i=i, w_next=w_next, w_prior=w_prior):
            own = [m[i, c, z] for c in range(3)]
            ahead = [m[1, c, z] if i == 0 else nxt[c, z] for c in range(3)]
            behind = [prior[c, z] if i == 0 else m[0, c, z] for c in range(3)]
            v = [
                w_next * (ahead[c] - own[c]) + w_prior * (own[c] - behind[c]) for c in range(3)
            ]
            along = v[0] * own[0] + v[1] * own[1] + v[2] * own[2]
            for c in range(3):
                t = v[c] - along * own[c]
                tang[i, c, z] = t
                acc = acc + t * t
            return acc

        lengths.append(total(lax.fori_loop(0, NZ, tangent, flat)))

    for t in range(2):
        @pl.when(me != (1 - t) * NZ)
        def _(t=t):
            wait_bytes(hbuf.at[t], g_r.at[t])

    def add_halves(image, c, sign, values):
        for n in range(NZ // 2):
            floc[image, c, n] = floc[image, c, n] + values[n]
            floc[image, c, NZ - 1 - n] = floc[image, c, NZ - 1 - n] + sign * values[n]

    def own_result(j):
        sign = jnp.where(part_of(j) == 0, 1.0, -1.0)
        c = j % 3

        def put(n, value):
            floc[hi, c, n] = floc[hi, c, n] + value
            floc[hi, c, NZ - 1 - n] = floc[hi, c, NZ - 1 - n] + sign * value

        half_layers(0, j, put)
        result_copy(j).wait_recv()
        add_halves(1 - hi, c, sign, [rbuf[j, n] for n in range(NZ // 2)])

    def extra_result(c):
        add_halves(0, c, -1.0, [hbuf[0, c] * layer_wave(NZ, n, True) for n in range(NZ // 2)])
        add_halves(1, c, 1.0, [hbuf[1, c] * layer_wave(0, n, False) for n in range(NZ // 2)])

    each(0, 3, extra_result)
    each(0, 6, own_result)

    drives = []
    for i in range(2):
        def force(z, acc, i=i):
            own = [m[i, c, z] for c in range(3)]
            f = [floc[i, c, z] for c in range(3)]
            along = f[0] * own[0] + f[1] * own[1] + f[2] * own[2]
            for c in range(3):
                t = f[c] - along * own[c]
                floc[i, c, z] = t
                acc = acc + t * tang[i, c, z]
            return acc

        drives.append(total(lax.fori_loop(0, NZ, force, flat)))

    send_round(round_c, msg_c, got_c, line_of(lengths + drives + spans))
    round_c[1]()
    sums = sum_round(got_c)
    dist = [jnp.sqrt(sums[0:1, 4 + j : 5 + j] / CELLS) for j in range(3)]
    tops = []
    for i in range(2):
        scale = jnp.sqrt(sums[0:1, i : i + 1] / CELLS + epsilon)
        parallel = sums[0:1, 2 + i : 3 + i] / (CELLS * scale)
        spring = spring_strength * (dist[i + 1] - dist[i])
        index = 2 * im + i
        interior = (index > 0) & (index < 2 * images - 1)
        coef = jnp.broadcast_to((spring - parallel) / scale, (NROW, NY))
        inner = jnp.where(interior, 1, 0)

        def band(z, acc, i=i, coef=coef, inner=inner):
            size = None
            for c in range(3):
                b = floc[i, c, z] + coef * tang[i, c, z]
                b = jnp.where(inner > 0, b, 0.0)
                out_b[i, c, z] = b
                size = b * b if size is None else size + b * b
            return jnp.maximum(acc, size)

        top = lax.fori_loop(0, NZ, band, flat)
        tops.append(jnp.max(jnp.max(top, axis=0, keepdims=True), axis=1, keepdims=True))

    send_round(round_d, msg_d, got_d, line_of(tops))
    round_d[1]()
    largest = got_d[0]
    for s in range(1, SPACE):
        largest = jnp.maximum(largest, got_d[s])
    largest = jnp.sqrt(largest)
    tile_x[1] = largest

    def drain(k):
        @pl.when(near(k) % NZ != 0)
        def _():
            wait_bytes(sbuf.at[0, pl.ds(0, 2)], y_s.at[k])

        @pl.when(near(k) % NZ == 0)
        def _():
            wait_bytes(sbuf.at[0, 0], y_s.at[k])

        @pl.when(special)
        def _():
            wait_bytes(sbuf.at[0, 0], f_s.at[k])

        @pl.when(jnp.logical_not(special))
        def _():
            wait_bytes(sbuf.at[0, pl.ds(0, 2)], f_s.at[k])

    each(1, NZ, drain)

    @pl.when(special)
    def _():
        wait_bytes(fbuf.at[pl.ds(0, 3), pl.ds(0, SPACE - 1)], g_s)

    for t in range(2):
        @pl.when(me != t * NZ)
        def _(t=t):
            wait_bytes(xbuf.at[t], x_s.at[t])

    each(0, 6, lambda j: partner_copy(j).wait_send())
    each(0, 6, lambda j: result_copy(j).wait_send())
    for rnd in (round_c, round_d):
        rnd[2]()
    wait_bytes(mine, e_s)
    at_images(lambda other, slot: wait_bytes(got_e.at[2 * slot], n_s.at[slot]))
    at_images(lambda other, slot: image_copy(other, slot).wait_send())
    at_slabs(lambda side: halo_copy(side).wait_send())


def finish_kernel(m_ref, b_ref, tile_ref, upd_hbm, bf_hbm, en_ref, upd, sem):
    stores = [pltpu.make_async_copy(b_ref, bf_hbm, sem.at[2])]
    stores[0].start()
    for i in range(2):
        en_ref[i] = jnp.max(tile_ref[0, :, i : i + 1])
        move = jnp.minimum(
            step_limit, rotation_limit / (tile_ref[1, :, i : i + 1] + epsilon)
        )
        move = jnp.broadcast_to(move, (NROW, NY))

        def advance(z, carry, i=i, move=move):
            s = [m_ref[i, c, z] + move * b_ref[i, c, z] for c in range(3)]
            length = jnp.sqrt(s[0] * s[0] + s[1] * s[1] + s[2] * s[2])
            for c in range(3):
                upd[i, c, z] = s[c] / length
            return carry

        lax.fori_loop(0, NZ, advance, 0)
        stores.append(pltpu.make_async_copy(upd.at[i], upd_hbm.at[i], sem.at[i]))
        stores[-1].start()
    for c in stores:
        c.wait()


def body(magnet, anisotropy, kernel):
    table = wave_table(NX)
    across = np.concatenate(split_table(np.ascontiguousarray(table.T)), axis=1)
    tables = jnp.asarray(np.concatenate([*split_table(table), across], axis=0))
    slab = (2, 3, NZ, NROW, NY)
    vm = pltpu.VMEM
    dma = pltpu.SemaphoreType.DMA
    tile = (1, 128)
    scratch = [
        vm(slab[1:], F32), vm(slab[1:], F32),
        vm((2, 2, 3, NZ, NY), F32), vm((2, 2, 3, NZ, NY), F32),
        vm((6, NZ // 2, NROW, NY), F32), vm((6, NZ // 2, NROW, NY), F32), vm((2, 3, NROW, NY), F32),
        vm((2, NZ, 6, NROW, NY), F32), vm((6, SPACE, NROW, NY), F32),
        vm((NX, 2 * NY), BF16), vm((NX, 2 * NY), BF16),
        vm((6, 2 * NX, 2 * NY), F32),
        vm((6, 2 * NX, 2 * NY), BF16), vm((6, 2 * NX, 2 * NY), BF16),
        vm((6, NX + 8, NY + 128), F32), vm((6, 2 * NX, 2 * NY), F32),
        vm((2 * NX, 2 * NY), BF16),
        vm((6, SPACE, NROW, NY), F32), vm((2, 6, NZ, NROW, NY), F32),
        vm((6, NZ // 2, NROW, NY), F32), vm((6, NZ // 2, NROW, NY), F32), vm((2, 3, NROW, NY), F32),
        vm(slab, F32), vm(slab, F32),
        vm((2 * NX, 2 * NY), BF16), vm((2, 2 * NX, NY), BF16), pltpu.SMEM((NROW,), F32),
        vm(tile, F32), vm((3, SPACE, *tile), F32),
        vm(tile, F32), vm((SPACE, *tile), F32),
        vm(tile, F32), vm((SPACE, *tile), F32),
        dma((6,)),
        dma((6,)), dma((6,)), dma((2,)), dma((3,)),
        dma((NZ,)), dma((6,)), dma((NZ,)), dma((2, 6)), dma, dma((2,)), dma((6,)), dma((6,)),
        dma, dma, dma((2,)), dma((2,)), dma, dma, dma, dma,
        dma((2,)), dma((2,)), dma((2,)), dma((2,)),
    ]
    hbm = pl.BlockSpec(memory_space=pltpu.HBM)
    vmem = pl.BlockSpec(memory_space=pltpu.VMEM)
    smem = pl.BlockSpec(memory_space=pltpu.SMEM)
    own, band, tiles = pl.pallas_call(
        step_kernel,
        out_shape=(
            jax.ShapeDtypeStruct(slab, F32),
            jax.ShapeDtypeStruct(slab, F32),
            jax.ShapeDtypeStruct((2, *tile), F32),
        ),
        in_specs=[hbm] * 4,
        out_specs=(vmem, vmem, vmem),
        scratch_shapes=scratch,
        compiler_params=pltpu.CompilerParams(
            collective_id=0, has_side_effects=True, vmem_limit_bytes=STEP_VMEM
        ),
        name="band_step",
    )(magnet, anisotropy, kernel, tables)
    return pl.pallas_call(
        finish_kernel,
        out_shape=(
            jax.ShapeDtypeStruct(slab, F32),
            jax.ShapeDtypeStruct(slab, F32),
            jax.ShapeDtypeStruct((2,), F32),
        ),
        in_specs=[vmem, vmem, vmem],
        out_specs=(hbm, hbm, smem),
        scratch_shapes=[vm(slab, F32), dma((3,))],
        compiler_params=pltpu.CompilerParams(vmem_limit_bytes=3 * 2**20),
        name="band_finish",
    )(own, band, tiles)


def solution(mesh):
    in_specs = (P("image", None, None, "space", None), P("space"), P(None, "space", None, None))
    out_specs = (
        P("image", None, None, "space", None),
        P("image", None, None, "space", None),
        P("image"),
    )
    return jax.shard_map(body, mesh=mesh, in_specs=in_specs, out_specs=out_specs, check_vma=False)
```
